32 devices in a mesh: rep: 4 (over x, y), dp: 8 (over z, core).
Axes of the slice: x: 2, y: 2, z: 4, core: 2. Of those that a mesh axis runs over, the one named last changes fastest.
Arguments:
- x: bfloat16 [32, 2048, 896], P(('rep', 'dp')), parts along dimension 0
- dy: bfloat16 [32, 2048, 896], P(('rep', 'dp')), parts along dimension 0
- w_gate: bfloat16 [2, 896, 2304], replicated
- w_up: bfloat16 [2, 896, 2304], replicated
- w_down: bfloat16 [2, 2304, 896], replicated
- m_w_gate: float32 [2, 896, 2304], P(None, 'dp')
- m_w_up: float32 [2, 896, 2304], P(None, 'dp')
- m_w_down: float32 [2, 2304, 896], P(None, 'dp')
- v_w_gate: float32 [2, 896, 2304], P(None, 'dp')
- v_w_up: float32 [2, 896, 2304], P(None, 'dp')
- v_w_down: float32 [2, 2304, 896], P(None, 'dp')
Outputs:
- output 1: bfloat16 [8, 896, 2304], P('rep'), parts along dimension 0
- output 2: bfloat16 [8, 896, 2304], P('rep'), parts along dimension 0
- output 3: bfloat16 [8, 2304, 896], P('rep'), parts along dimension 0
- output 4: float32 [8, 896, 2304], P('rep', 'dp'), parts along dimension 0
- output 5: float32 [8, 896, 2304], P('rep', 'dp'), parts along dimension 0
- output 6: float32 [8, 2304, 896], P('rep', 'dp'), parts along dimension 0
- output 7: float32 [8, 896, 2304], P('rep', 'dp'), parts along dimension 0
- output 8: float32 [8, 896, 2304], P('rep', 'dp'), parts along dimension 0
- output 9: float32 [8, 2304, 896], P('rep', 'dp'), parts along dimension 0
There are 4 independent parts. The reference program is written for one: setup_inputs(seed, part) draws one part's arguments, and reference() takes and returns one part's arrays. A program takes and returns all parts, laid end to end along the dimension named above; an argument that names none is the same for every part.
All inputs are finite; a program needn't handle non-finite values.
Results may differ from the reference program's by a relative error of at most 0.02.
Values are sent between devices in bfloat16 or wider.
A program may use at most 2 GiB of HBM per device.

```python
import jax
import jax.numpy as jnp
from jax import lax

SEQUENCES = 8
TOKENS = 2048
D = 896
FF = 2304
LAYERS = 2
NAMES = ("w_gate", "w_up", "w_down")
SHAPES = {"w_gate": (LAYERS, D, FF), "w_up": (LAYERS, D, FF), "w_down": (LAYERS, FF, D)}


def bump(key, n, height):
    away = (jnp.arange(n, dtype=jnp.int32) - jax.random.randint(key, (), 0, n, jnp.int32)) % n
    return jnp.where(away < n // 8, height, 1.0)


def together(key, own, strength):
    shared = jax.random.normal(key, own.shape[1:], jnp.float32)
    return (own + strength * shared) * lax.rsqrt(1 + strength * strength)


def setup_inputs(seed: int = 0, part: int = 0) -> dict:
    kx, kdy, ka, kb, kz, kf, kh, kl, *keys = jax.random.split(jax.random.key(seed), 8 + 3 * len(NAMES))
    kx, kdy, ka, kb = (jax.random.fold_in(k, part) for k in (kx, kdy, ka, kb))
    kw, km, kv = (keys[i::3] for i in range(3))
    shape = (SEQUENCES, TOKENS, D)
    much_x, much_dy = jax.random.uniform(kz, (2,), jnp.float32, 0.0, 1.0)
    loud = 2.0 ** jax.random.uniform(jax.random.fold_in(kz, 1), (), jnp.float32, -1.0, 2.0)
    layers = 2.0 ** jax.random.uniform(kl, (LAYERS, 1, 1), jnp.float32, -1.0, 1.0)
    x = together(ka, jax.random.normal(kx, shape, jnp.float32), much_x) * bump(kf, D, 4.0)
    dy = together(kb, jax.random.normal(kdy, shape, jnp.float32), much_dy)
    drawn = {"x": x.astype(jnp.bfloat16), "dy": (loud * dy * (SEQUENCES * TOKENS) ** -0.5).astype(jnp.bfloat16)}
    for key, name in zip(kw, NAMES, strict=True):
        w = jax.random.normal(key, SHAPES[name], jnp.float32) * SHAPES[name][1] ** -0.5
        drawn[name] = (w * {"w_gate": 1.0, "w_up": bump(kh, FF, 4.0), "w_down": layers}[name]).astype(jnp.bfloat16)
    for key, name in zip(km, NAMES, strict=True):
        drawn[f"m_{name}"] = 0.1 * jax.random.normal(key, SHAPES[name], jnp.float32)
    for key, name in zip(kv, NAMES, strict=True):
        drawn[f"v_{name}"] = jax.random.uniform(key, SHAPES[name], jnp.float32, 0.005, 0.015)
    return drawn


def matmul(a, w):
    return jnp.dot(a, w, preferred_element_type=jnp.float32).astype(jnp.bfloat16)


def normed(h):
    wide = h.astype(jnp.float32)
    scale = lax.rsqrt(jnp.mean(wide**2, -1, keepdims=True) + 1e-6)
    return (wide * scale).astype(jnp.bfloat16)


def layer(h, w):
    a = normed(h)
    gate = jnp.dot(a, w["w_gate"], preferred_element_type=jnp.float32)
    up = jnp.dot(a, w["w_up"], preferred_element_type=jnp.float32)
    return h + matmul((jax.nn.silu(gate) * up).astype(jnp.bfloat16), w["w_down"])


def adamw(w, m, v, g):
    m = 0.9 * m + 0.1 * g
    v = 0.95 * v + 0.05 * g * g
    step = m * lax.rsqrt(v + 1e-8) + 0.1 * w
    return (w - 0.02 * step).astype(jnp.bfloat16), m, v


def stack(weights, h):
    return lax.scan(lambda h, w: (layer(h, w), None), h, weights)[0]


def reference(x, dy, w_gate, w_up, w_down, m_w_gate, m_w_up, m_w_down, v_w_gate, v_w_up, v_w_down):
    weights = dict(zip(NAMES, (w_gate, w_up, w_down), strict=True))

    def take(so_far, sequence):
        h, by_y = sequence
        _, back = jax.vjp(lambda w: stack(w, h), weights)
        return jax.tree.map(lambda total, term: total + term.astype(jnp.float32), so_far, back(by_y)[0]), None

    none_yet = {name: jnp.zeros(w.shape, jnp.float32) for name, w in weights.items()}
    by_weights, _ = lax.scan(take, none_yet, (x, dy))
    gradients = [by_weights[name].astype(jnp.bfloat16).astype(jnp.float32) for name in NAMES]
    new = [
        adamw(w.astype(jnp.float32), m, v, g)
        for w, m, v, g in zip((w_gate, w_up, w_down), (m_w_gate, m_w_up, m_w_down), (v_w_gate, v_w_up, v_w_down), gradients, strict=True)
    ]
    return tuple(one[which] for which in range(3) for one in new)
```

```python
import functools

import jax
import jax.numpy as jnp
from jax import lax
from jax.experimental import pallas as pl
from jax.experimental.pallas import tpu as pltpu
from jax.sharding import PartitionSpec as P

MESH = pl.DeviceIdType.MESH
F32, BF16 = jnp.float32, jnp.bfloat16
T, D, FF = 2048, 896, 2304
CF = 256
STEPS = FF // CF
RB = 512
NRB = T // RB
ROWS = 224
PER_LAYER = 27
Q = 2 * PER_LAYER
RING = 12
SENDS = 4
LAST = Q + 18
VMEM_LIMIT = 67043328


def nt(a, b):
    return lax.dot_general(a, b, (((1,), (1,)), ((), ())), preferred_element_type=F32)


def nn(a, b):
    return jnp.dot(a, b, preferred_element_type=F32)


def norm_scale(wide):
    return lax.rsqrt(jnp.mean(wide * wide, -1, keepdims=True) + 1e-6)


def sigmoid(g):
    return 1.0 / (1.0 + jnp.exp(-g))


def forward_kernel(x, wg, wu, wd, g_out, u_out, hid_t, a0_t, h1, a1, a1_t, acc, a0):
    j = pl.program_id(0)

    @pl.when(j == 0)
    def _():
        @pl.loop(0, NRB)
        def _(r):
            rows = pl.ds(pl.multiple_of(r * RB, RB), RB)
            wide = x[rows, :].astype(F32)
            a = (wide * norm_scale(wide)).astype(BF16)
            a0[rows, :] = a
            a0_t[:, rows] = a.T

    @pl.loop(0, NRB)
    def _(r):
        rows = pl.ds(pl.multiple_of(r * RB, RB), RB)
        a = a0[rows, :]
        g = nn(a, wg[0])
        u = nn(a, wu[0])
        g_out[0, rows, :] = g
        u_out[0, rows, :] = u
        hid = (g * sigmoid(g) * u).astype(BF16)
        hid_t[:, :, rows] = hid.T.reshape(8, 32, RB)
        y = nn(hid, wd[0])

        @pl.when(j == 0)
        def _():
            acc[rows, :] = y

        @pl.when(j > 0)
        def _():
            acc[rows, :] += y

    @pl.when(j == STEPS - 1)
    def _():
        @pl.loop(0, NRB)
        def _(r):
            rows = pl.ds(pl.multiple_of(r * RB, RB), RB)
            y = acc[rows, :].astype(BF16).astype(F32)
            h = (x[rows, :].astype(F32) + y).astype(BF16)
            h1[rows, :] = h
            wide = h.astype(F32)
            a = (wide * norm_scale(wide)).astype(BF16)
            a1[rows, :] = a
            a1_t[:, rows] = a.T


def forward(x, wg, wu, wd):
    whole = lambda *shape: pl.BlockSpec(shape, lambda j: (0,) * len(shape), pipeline_mode=pl.Buffered(1))
    step = lambda *shape: pl.BlockSpec(shape, lambda j: (j,) + (0,) * (len(shape) - 1))
    return pl.pallas_call(
        forward_kernel,
        grid=(STEPS,),
        in_specs=[
            whole(T, D),
            pl.BlockSpec((1, D, CF), lambda j: (0, 0, j)),
            pl.BlockSpec((1, D, CF), lambda j: (0, 0, j)),
            pl.BlockSpec((1, CF, D), lambda j: (0, j, 0)),
        ],
        out_specs=[step(1, T, CF), step(1, T, CF), step(8, 32, T), whole(D, T), whole(T, D), whole(T, D), whole(D, T)],
        out_shape=[
            jax.ShapeDtypeStruct((STEPS, T, CF), F32),
            jax.ShapeDtypeStruct((STEPS, T, CF), F32),
            jax.ShapeDtypeStruct((72, 32, T), BF16),
            jax.ShapeDtypeStruct((D, T), BF16),
            jax.ShapeDtypeStruct((T, D), BF16),
            jax.ShapeDtypeStruct((T, D), BF16),
            jax.ShapeDtypeStruct((D, T), BF16),
        ],
        scratch_shapes=[pltpu.VMEM((T, D), F32), pltpu.VMEM((T, D), BF16)],
        compiler_params=pltpu.CompilerParams(vmem_limit_bytes=VMEM_LIMIT, dimension_semantics=("arbitrary",)),
        name="forward0",
    )(x, wg, wu, wd)


def train_kernel(
    wg, wu, wd, mg, mu, md, vg, vu, vd, dy, h1, a1, a1_t, a0_t, hid0_t, g0, u0,
    wtmp, gown, hid1_t,
    dyv, av, at, gbuf, ubuf, dg, du, wgj, wuj, wdj, hid_b, hid_c, dag, dau,
    grad, pin, rin, lin, rout, lout, wown, gownb, gfin, mb, vb, wb, mbd, vbd, wbd,
    load_sem, w_sem, gu_sem, hw_sem, hc_sem,
    p_send, p_recv, r_send, r_recv, l_send, l_recv,
    ar_send, ar_recv, al_send, al_recv, ap_send, ap_recv, wo_sem, go_sem, ad_sem,
):
    rep, me = lax.axis_index("rep"), lax.axis_index("dp")
    z, c = me // 2, me % 2
    partner = (rep, z * 2 + (1 - c))
    right = (rep, jnp.minimum(z + 1, 3) * 2 + c)
    left = (rep, jnp.maximum(z - 1, 0) * 2 + c)

    bar = pltpu.get_barrier_semaphore()
    pl.semaphore_signal(bar, inc=1, device_id=partner, device_id_type=MESH)

    @pl.when(z < 3)
    def _():
        pl.semaphore_signal(bar, inc=1, device_id=right, device_id_type=MESH)

    @pl.when(z > 0)
    def _():
        pl.semaphore_signal(bar, inc=1, device_id=left, device_id_type=MESH)

    @pl.when((z == 0) | (z == 3))
    def _():
        pl.semaphore_wait(bar, 2)

    @pl.when((z > 0) & (z < 3))
    def _():
        pl.semaphore_wait(bar, 3)

    valid = lambda q: (q >= 0) & (q < Q)

    def remote(src, dst, send, recv, to):
        return pltpu.make_async_remote_copy(
            src_ref=src, dst_ref=dst, send_sem=send, recv_sem=recv, device_id=to, device_id_type=MESH
        )

    def to_partner(q):
        return remote(grad.at[q % RING, 1 - c], pin.at[q % RING], p_send.at[q % SENDS], p_recv.at[q % RING], partner)

    def sum_right(q, frm):
        part = pl.ds(frm + 1, 3 - frm)
        return remote(rout.at[q % SENDS, part], rin.at[q % RING, part], r_send.at[q % SENDS], r_recv.at[q % RING], right)

    def sum_left(q, frm):
        part = pl.ds(0, frm)
        return remote(lout.at[q % SENDS, part], lin.at[q % RING, part], l_send.at[q % SENDS], l_recv.at[q % RING], left)

    def new_right(q, frm):
        part = pl.ds(0, frm + 1)
        here = wtmp.at[q, c, part]
        return remote(here, here, ar_send.at[q % SENDS], ar_recv.at[q % RING], right)

    def new_left(q, frm):
        part = pl.ds(frm, 4 - frm)
        here = wtmp.at[q, c, part]
        return remote(here, here, al_send.at[q % SENDS], al_recv.at[q % RING], left)

    def new_partner(q, core):
        here = wtmp.at[q, core]
        return remote(here, here, ap_send.at[q % SENDS], ap_recv.at[q % RING], partner)

    def keep_new(q):
        return pltpu.make_async_copy(wown.at[q % SENDS], wtmp.at[q, c, z], wo_sem.at[q % SENDS])

    def keep_grad(q):
        return pltpu.make_async_copy(gownb.at[q % SENDS], gown.at[q], go_sem.at[q % SENDS])

    def moments(q, act):
        layer = jnp.where(q < PER_LAYER, 1, 0)
        n = q % PER_LAYER
        s = q % 2
        cols = pl.ds(pl.multiple_of((n // 2) * CF, CF), CF)
        for which, (m, v, w) in enumerate(((mg, vg, wg), (mu, vu, wu))):

            @pl.when((n < 18) & (n % 2 == which))
            def _():
                own = pl.ds(pl.multiple_of(me * 112, 16), 112)
                act(pltpu.make_async_copy(m.at[layer, :, cols], mb.at[s], ad_sem.at[s, 0]))
                act(pltpu.make_async_copy(v.at[layer, :, cols], vb.at[s], ad_sem.at[s, 1]))
                act(pltpu.make_async_copy(w.at[layer, own, cols], wb.at[s], ad_sem.at[s, 2]))

        @pl.when(n >= 18)
        def _():
            rows = pl.ds(pl.multiple_of((n - 18) * 32, 32), 32)
            own = pl.ds(pl.multiple_of(me * 288 + (n - 18) * 32, 32), 32)
            act(pltpu.make_async_copy(md.at[layer, rows, :], mbd.at[s], ad_sem.at[s, 0]))
            act(pltpu.make_async_copy(vd.at[layer, rows, :], vbd.at[s], ad_sem.at[s, 1]))
            act(pltpu.make_async_copy(wd.at[layer, own, :], wbd.at[s], ad_sem.at[s, 2]))

    def new_weight(w, m, v, g):
        m = 0.9 * m + 0.1 * g
        v = 0.95 * v + 0.05 * g * g
        step = m * lax.rsqrt(v + 1e-8) + 0.1 * w
        return (w - 0.02 * step).astype(BF16)

    def weights_of(n, act):
        s = n % 2

        @pl.when(n < STEPS)
        def _():
            cols = pl.ds(pl.multiple_of(n * CF, CF), CF)
            act(pltpu.make_async_copy(wg.at[1, :, cols], wgj.at[s], w_sem.at[s, 0]))
            act(pltpu.make_async_copy(wu.at[1, :, cols], wuj.at[s], w_sem.at[s, 1]))
            act(pltpu.make_async_copy(wd.at[1, cols, :], wdj.at[s], w_sem.at[s, 2]))

        @pl.when((n >= STEPS) & (n < 2 * STEPS))
        def _():
            cols = pl.ds(pl.multiple_of((n - STEPS) * CF, CF), CF)
            act(pltpu.make_async_copy(wd.at[0, cols, :], wdj.at[s], w_sem.at[s, 2]))

    def saved_of(n, act):
        @pl.when((n >= STEPS) & (n < 2 * STEPS))
        def _():
            act(pltpu.make_async_copy(g0.at[n - STEPS], gbuf, gu_sem.at[0]))
            act(pltpu.make_async_copy(u0.at[n - STEPS], ubuf, gu_sem.at[1]))

    def keep_hidden(j):
        return pltpu.make_async_copy(hid_b, hid1_t.at[pl.ds(j * 8, 8)], hw_sem)

    def hidden_of(src, k, start):
        s = k % 2
        if start:
            for o in range(8):
                pltpu.make_async_copy(src.at[o * 9 + k], hid_c.at[s, o], hc_sem.at[s]).start()
        else:
            pltpu.make_async_copy(src.at[pl.ds(0, 8)], hid_c.at[s], hc_sem.at[s]).wait()

    whole = [
        pltpu.make_async_copy(dy, dyv, load_sem.at[0]),
        pltpu.make_async_copy(a1, av, load_sem.at[1]),
        pltpu.make_async_copy(a1_t, at, load_sem.at[2]),
    ]
    second_h = pltpu.make_async_copy(h1, av, load_sem.at[1])
    second_at = pltpu.make_async_copy(a0_t, at, load_sem.at[2])

    start = lambda copy: copy.start()
    wait = lambda copy: copy.wait()

    def grad_columns(q, d):
        @pl.loop(0, 2)
        def _(half):
            rows = pl.ds(pl.multiple_of(half * 448, 448), 448)
            out = nn(at[rows, :], d[...]).astype(BF16)
            for o in range(4):
                for h in range(2):
                    grad[q % RING, o % 2, half * 2 + o // 2, h * 112 : (h + 1) * 112, :] = out[
                        o * 112 : (o + 1) * 112, h * 128 : (h + 1) * 128
                    ]

    def grad_rows(q, k, d):
        out = nn(hid_c[k % 2].reshape(256, T), d[...]).astype(BF16)
        for o in range(8):
            for h in range(7):
                grad[q % RING, o % 2, o // 2, h * 32 : (h + 1) * 32, :] = out[
                    o * 32 : (o + 1) * 32, h * 128 : (h + 1) * 128
                ]

    def hidden_back(g, u, dp):
        s = sigmoid(g)
        act = g * s
        return act, (dp * u * (s + act * (1.0 - s))).astype(BF16), (dp * act).astype(BF16)

    def compute(s):
        @pl.when((s < 18) & (s % 2 == 0))
        def _():
            j = s // 2
            b = j % 2
            weights_of(j + 1, start)
            weights_of(j, wait)

            @pl.when(j == 0)
            def _():
                for copy in whole:
                    copy.wait()

            @pl.when(j > 0)
            def _():
                keep_hidden(j - 1).wait()

            @pl.loop(0, NRB)
            def _(r):
                rows = pl.ds(pl.multiple_of(r * RB, RB), RB)
                a = av[rows, :]
                g = nn(a, wgj[b])
                u = nn(a, wuj[b])
                dp = nt(dyv[rows, :], wdj[b]).astype(BF16).astype(F32)
                act, dgr, dur = hidden_back(g, u, dp)
                hid_b[:, :, rows] = (act * u).astype(BF16).T.reshape(8, 32, RB)
                dg[rows, :] = dgr
                du[rows, :] = dur

            keep_hidden(j).start()
            grad_columns(s, dg)

            @pl.when(j == STEPS - 1)
            def _():
                second_h.start()

        @pl.when((s < 18) & (s % 2 == 1))
        def _():
            j = s // 2
            b = j % 2
            grad_columns(s, du)

            @pl.loop(0, NRB)
            def _(r):
                rows = pl.ds(pl.multiple_of(r * RB, RB), RB)
                by_g = nt(dg[rows, :], wgj[b])
                by_u = nt(du[rows, :], wuj[b])

                @pl.when(j == 0)
                def _():
                    dag[rows, :] = by_g
                    dau[rows, :] = by_u

                @pl.when(j > 0)
                def _():
                    dag[rows, :] += by_g
                    dau[rows, :] += by_u

            @pl.when(j == STEPS - 1)
            def _():
                keep_hidden(j).wait()
                hidden_of(hid1_t, 0, True)
                second_at.start()
                second_h.wait()

                @pl.loop(0, T // 128)
                def _(r):
                    rows = pl.ds(pl.multiple_of(r * 128, 128), 128)
                    da = dag[rows, :].astype(BF16).astype(F32) + dau[rows, :].astype(BF16).astype(F32)
                    da = da.astype(BF16).astype(F32)
                    wide = av[rows, :].astype(F32)
                    scale = norm_scale(wide)
                    along = jnp.sum(da * wide, -1, keepdims=True) * (scale * scale * scale) * (-1.0 / D)
                    back = (da * scale + wide * along).astype(BF16)
                    av[rows, :] = (dyv[rows, :].astype(F32) + back.astype(F32)).astype(BF16)

        @pl.when((s >= 18) & (s < 27))
        def _():
            k = s - 18

            @pl.when(k < 8)
            def _():
                hidden_of(hid1_t, k + 1, True)

            hidden_of(hid1_t, k, False)
            grad_rows(s, k, dyv)

            @pl.when(k == 8)
            def _():
                second_at.wait()

        @pl.when((s >= 27) & (s < 45) & ((s - 27) % 2 == 0))
        def _():
            n = STEPS + (s - 27) // 2
            b = n % 2
            weights_of(n + 1, start)
            weights_of(n, wait)
            saved_of(n, wait)

            @pl.loop(0, NRB)
            def _(r):
                rows = pl.ds(pl.multiple_of(r * RB, RB), RB)
                dp = nt(av[rows, :], wdj[b]).astype(BF16).astype(F32)
                _, dgr, dur = hidden_back(gbuf[rows, :], ubuf[rows, :], dp)
                dg[rows, :] = dgr
                du[rows, :] = dur

            saved_of(n + 1, start)
            grad_columns(s, dg)

        @pl.when((s >= 27) & (s < 45) & ((s - 27) % 2 == 1))
        def _():
            grad_columns(s, du)

            @pl.when(s == 44)
            def _():
                hidden_of(hid0_t, 0, True)

        @pl.when((s >= 45) & (s < 54))
        def _():
            k = s - 45

            @pl.when(k < 8)
            def _():
                hidden_of(hid0_t, k + 1, True)

            hidden_of(hid0_t, k, False)
            grad_rows(s, k, av)

    f32 = lambda t: t.astype(F32)

    def exchange(s):
        q = s - 1

        @pl.when(valid(q))
        def _():
            to_partner(q).wait_recv()

        qr = s - 1 - 2 * z
        for zz in range(4):

            @pl.when(valid(qr) & (z == zz))
            def _():
                if zz > 0:
                    sum_right(qr, zz - 1).wait_recv()
                if zz < 3:

                    @pl.when(qr >= SENDS)
                    def _():
                        sum_right(qr - SENDS, zz).wait_send()

                    e = qr % RING
                    for to in range(zz + 1, 4):
                        t = f32(grad[e, c, to]) + f32(pin[e, to])
                        if zz > 0:
                            t = t + f32(rin[e, to])
                        rout[qr % SENDS, to] = t.astype(BF16)
                    sum_right(qr, zz).start()

        ql = s - 1 - 2 * (3 - z)
        for zz in range(4):

            @pl.when(valid(ql) & (z == zz))
            def _():
                if zz < 3:
                    sum_left(ql, zz + 1).wait_recv()
                if zz > 0:

                    @pl.when(ql >= SENDS)
                    def _():
                        sum_left(ql - SENDS, zz).wait_send()

                    e = ql % RING
                    for to in range(zz):
                        t = f32(grad[e, c, to]) + f32(pin[e, to])
                        if zz < 3:
                            t = t + f32(lin[e, to])
                        lout[ql % SENDS, to] = t.astype(BF16)
                    sum_left(ql, zz).start()

        for zz in range(4):

            @pl.when((qr >= Q) & (qr < Q + SENDS) & (z == zz))
            def _():
                if zz < 3:
                    sum_right(qr - SENDS, zz).wait_send()

            @pl.when((ql >= Q) & (ql < Q + SENDS) & (z == zz))
            def _():
                if zz > 0:
                    sum_left(ql - SENDS, zz).wait_send()

        @pl.when(valid(s - 6))
        def _():
            moments(s - 6, start)

        qf = s - 7

        @pl.when((qf >= SENDS) & (qf < Q + SENDS))
        def _():
            keep_grad(qf - SENDS).wait()

        @pl.when(valid(qf))
        def _():
            e, b = qf % RING, qf % SENDS
            gfin[...] = f32(grad[e, c, z]) + f32(pin[e, z])

            @pl.when(z > 0)
            def _():
                gfin[...] += f32(rin[e, z])

            @pl.when(z < 3)
            def _():
                gfin[...] += f32(lin[e, z])

            gownb[b] = gfin[...].astype(BF16)
            keep_grad(qf).start()
            moments(qf, wait)
            n = qf % PER_LAYER
            sl = qf % 2

            @pl.when(n < 18)
            def _():
                for h in range(2):
                    lanes = slice(h * 128, (h + 1) * 128)
                    part = slice(h * 112, (h + 1) * 112)
                    g = gownb[b, part, :].astype(F32)
                    wown[b, part, :] = new_weight(f32(wb[sl, :, lanes]), mb[sl, :, lanes], vb[sl, :, lanes], g)

            @pl.when(n >= 18)
            def _():
                for h in range(7):
                    lanes = slice(h * 128, (h + 1) * 128)
                    part = slice(h * 32, (h + 1) * 32)
                    g = gownb[b, part, :].astype(F32)
                    wown[b, part, :] = new_weight(f32(wbd[sl, :, lanes]), mbd[sl, :, lanes], vbd[sl, :, lanes], g)

            keep_new(qf).start()

        @pl.when(valid(s - 8))
        def _():
            keep_new(s - 8).wait()

        qar = s - 8 - 2 * z
        qal = s - 8 - 2 * (3 - z)
        for zz in range(4):

            @pl.when(valid(qar) & (z == zz))
            def _():
                if zz > 0:
                    new_right(qar, zz - 1).wait_recv()
                if zz < 3:

                    @pl.when(qar >= SENDS)
                    def _():
                        new_right(qar - SENDS, zz).wait_send()

                    new_right(qar, zz).start()

            @pl.when(valid(qal) & (z == zz))
            def _():
                if zz < 3:
                    new_left(qal, zz + 1).wait_recv()
                if zz > 0:

                    @pl.when(qal >= SENDS)
                    def _():
                        new_left(qal - SENDS, zz).wait_send()

                    new_left(qal, zz).start()

            @pl.when((qar >= Q) & (qar < Q + SENDS) & (z == zz))
            def _():
                if zz < 3:
                    new_right(qar - SENDS, zz).wait_send()

            @pl.when((qal >= Q) & (qal < Q + SENDS) & (z == zz))
            def _():
                if zz > 0:
                    new_left(qal - SENDS, zz).wait_send()

        qap = s - 14

        @pl.when((qap >= SENDS) & (qap < Q + SENDS))
        def _():
            new_partner(qap - SENDS, c).wait_send()

        @pl.when(valid(qap))
        def _():
            new_partner(qap, c).start()

        @pl.when(valid(s - 16))
        def _():
            new_partner(s - 16, 1 - c).wait_recv()

    for copy in whole:
        copy.start()
    weights_of(0, start)

    @pl.loop(0, LAST)
    def _(s):
        exchange(s)

        @pl.when(s < Q)
        def _():
            compute(s)

            @pl.when(s == 17)
            def _():
                saved_of(STEPS, start)

        @pl.when((s >= SENDS) & (s < Q + SENDS))
        def _():
            to_partner(s - SENDS).wait_send()

        @pl.when(s < Q)
        def _():
            to_partner(s).start()


def train(*operands):
    vm = pltpu.VMEM
    dma = pltpu.SemaphoreType.DMA
    any_ = pl.BlockSpec(memory_space=pl.ANY)
    return pl.pallas_call(
        train_kernel,
        in_specs=[any_] * len(operands),
        out_specs=[any_] * 3,
        out_shape=[
            jax.ShapeDtypeStruct((Q, 2, 4, ROWS, 128), BF16),
            jax.ShapeDtypeStruct((Q, ROWS, 128), BF16),
            jax.ShapeDtypeStruct((72, 32, T), BF16),
        ],
        scratch_shapes=[
            vm((T, D), BF16), vm((T, D), BF16), vm((D, T), BF16),
            vm((T, CF), F32), vm((T, CF), F32), vm((T, CF), BF16), vm((T, CF), BF16),
            vm((2, D, CF), BF16), vm((2, D, CF), BF16), vm((2, CF, D), BF16),
            vm((8, 32, T), BF16), vm((2, 8, 32, T), BF16),
            vm((T, D), F32), vm((T, D), F32),
            vm((RING, 2, 4, ROWS, 128), BF16), vm((RING, 4, ROWS, 128), BF16),
            vm((RING, 4, ROWS, 128), BF16), vm((RING, 4, ROWS, 128), BF16),
            vm((SENDS, 4, ROWS, 128), BF16), vm((SENDS, 4, ROWS, 128), BF16),
            vm((SENDS, ROWS, 128), BF16), vm((SENDS, ROWS, 128), BF16), vm((ROWS, 128), F32),
            vm((2, 112, CF), F32), vm((2, 112, CF), F32), vm((2, 112, CF), BF16),
            vm((2, 32, D), F32), vm((2, 32, D), F32), vm((2, 32, D), BF16),
            dma((3,)), dma((2, 3)), dma((2,)), dma, dma((2,)),
            dma((SENDS,)), dma((RING,)), dma((SENDS,)), dma((RING,)), dma((SENDS,)), dma((RING,)),
            dma((SENDS,)), dma((RING,)), dma((SENDS,)), dma((RING,)), dma((SENDS,)), dma((RING,)),
            dma((SENDS,)), dma((SENDS,)), dma((2, 3)),
        ],
        compiler_params=pltpu.CompilerParams(
            collective_id=0, has_side_effects=True, vmem_limit_bytes=VMEM_LIMIT
        ),
        name="train",
    )(*operands)


def finish_kernel(wt_g, wt_u, wt_d, gg, gu, gd, mg, mu, md, vg, vu, vd, owg, owu, owd, omg, omu, omd, ovg, ovu, ovd):
    for src, dst in ((wt_g, owg), (wt_u, owu)):
        for o in range(8):
            for h in range(2):
                dst[0, o * 112 : (o + 1) * 112, h * 128 : (h + 1) * 128] = src[0, o % 2, o // 2, h * 112 : (h + 1) * 112, :]
    for o in range(8):
        for h in range(7):
            owd[0, o, :, h * 128 : (h + 1) * 128] = wt_d[0, o % 2, o // 2, h * 32 : (h + 1) * 32, :]
    for g, m, v, om, ov, n, rows in ((gg, mg, vg, omg, ovg, 2, 112), (gu, mu, vu, omu, ovu, 2, 112), (gd, md, vd, omd, ovd, 7, 32)):
        for h in range(n):
            lanes = slice(h * 128, (h + 1) * 128)
            gr = g[0, h * rows : (h + 1) * rows, :].astype(F32)
            om[0, :, lanes] = 0.9 * m[0, :, lanes] + 0.1 * gr
            ov[0, :, lanes] = 0.95 * v[0, :, lanes] + 0.05 * gr * gr


def finish(wtmp, gown, m, v):
    layer = lambda i: i // STEPS
    first = lambda i: (1 - i // STEPS) * PER_LAYER
    chunk = (lambda i: first(i) + 2 * (i % STEPS), lambda i: first(i) + 2 * (i % STEPS) + 1, lambda i: first(i) + 18 + i % STEPS)
    blocks = [pl.BlockSpec((1, 2, 4, ROWS, 128), functools.partial(lambda f, i: (f(i), 0, 0, 0, 0), f)) for f in chunk]
    grads = [pl.BlockSpec((1, ROWS, 128), functools.partial(lambda f, i: (f(i), 0, 0), f)) for f in chunk]
    cols = pl.BlockSpec((1, 112, CF), lambda i: (layer(i), 0, i % STEPS))
    rows = pl.BlockSpec((1, 32, D), lambda i: (layer(i), i % STEPS, 0))
    wcols = pl.BlockSpec((1, D, CF), lambda i: (layer(i), 0, i % STEPS))
    wrows = pl.BlockSpec((1, 8, 32, D), lambda i: (layer(i), 0, i % STEPS, 0))
    out = pl.pallas_call(
        finish_kernel,
        grid=(2 * STEPS,),
        in_specs=[*blocks, *grads, cols, cols, rows, cols, cols, rows],
        out_specs=[wcols, wcols, wrows, cols, cols, rows, cols, cols, rows],
        out_shape=[
            jax.ShapeDtypeStruct((2, D, FF), BF16), jax.ShapeDtypeStruct((2, D, FF), BF16),
            jax.ShapeDtypeStruct((2, 8, 288, D), BF16),
            *[jax.ShapeDtypeStruct(t.shape, F32) for t in (*m, *v)],
        ],
        compiler_params=pltpu.CompilerParams(vmem_limit_bytes=VMEM_LIMIT, dimension_semantics=("arbitrary",)),
        name="finish",
    )(wtmp, wtmp, wtmp, gown, gown, gown, *m, *v)
    return (out[0], out[1], out[2].reshape(2, FF, D), *out[3:])


def solution(mesh):
    def step(x, dy, wg, wu, wd, *moments):
        m, v = moments[:3], moments[3:]
        g0, u0, hid0_t, a0_t, h1, a1, a1_t = forward(x[0], wg, wu, wd)
        wtmp, gown, _ = train(wg, wu, wd, *m, *v, dy[0], h1, a1, a1_t, a0_t, hid0_t, g0, u0)
        return finish(wtmp, gown, m, v)

    seq, whole, rows = P(("rep", "dp")), P(), P(None, "dp")
    return jax.shard_map(
        step, mesh=mesh,
        in_specs=(seq, seq, *[whole] * 3, *[rows] * 6),
        out_specs=(*[P("rep")] * 3, *[P("rep", "dp")] * 6),
        check_vma=False,
    )
```

```python
import functools

import jax
import jax.numpy as jnp
from jax import lax
from jax.experimental import pallas as pl
from jax.experimental.pallas import tpu as pltpu
from jax.sharding import PartitionSpec as P

MESH = pl.DeviceIdType.MESH
F32, BF16 = jnp.float32, jnp.bfloat16
T, D, FF = 2048, 896, 2304
CF = 256
STEPS = FF // CF
RB = 512
NRB = T // RB
ROWS = 224
PER_LAYER = 27
Q = 2 * PER_LAYER
RING = 12
SENDS = 4
LAST = Q + 18
VMEM_LIMIT = 67043328


def nt(a, b):
    return lax.dot_general(a, b, (((1,), (1,)), ((), ())), preferred_element_type=F32)


def nn(a, b):
    return jnp.dot(a, b, preferred_element_type=F32)


def norm_scale(wide):
    return lax.rsqrt(jnp.mean(wide * wide, -1, keepdims=True) + 1e-6)


def sigmoid(g):
    return 1.0 / (1.0 + jnp.exp(-g))


def train_kernel(
    wg, wu, wd, mg, mu, md, vg, vu, vd, x, dy,
    wtmp, gown, hid0_t, hid1_t, a0_t, g0, u0, dg1, du1,
    xv, dyv, av, at, gbuf, ubuf, dg, du, wgj, wuj, wdj, hid_b, hid_c,
    grad, pin, rin, lin, rout, lout, wown, gownb, gfin, mb, vb, wb, mbd, vbd, wbd,
    load_sem, w_sem, gu_sem, keep_sem, hw_sem, hc_sem, d_sem, da_sem,
    p_send, p_recv, r_send, r_recv, l_send, l_recv,
    ar_send, ar_recv, al_send, al_recv, ap_send, ap_recv, wo_sem, go_sem, ad_sem,
):
    rep, me = lax.axis_index("rep"), lax.axis_index("dp")
    z, c = me // 2, me % 2
    partner = (rep, z * 2 + (1 - c))
    right = (rep, jnp.minimum(z + 1, 3) * 2 + c)
    left = (rep, jnp.maximum(z - 1, 0) * 2 + c)

    bar = pltpu.get_barrier_semaphore()
    pl.semaphore_signal(bar, inc=1, device_id=partner, device_id_type=MESH)

    @pl.when(z < 3)
    def _():
        pl.semaphore_signal(bar, inc=1, device_id=right, device_id_type=MESH)

    @pl.when(z > 0)
    def _():
        pl.semaphore_signal(bar, inc=1, device_id=left, device_id_type=MESH)

    @pl.when((z == 0) | (z == 3))
    def _():
        pl.semaphore_wait(bar, 2)

    @pl.when((z > 0) & (z < 3))
    def _():
        pl.semaphore_wait(bar, 3)

    valid = lambda q: (q >= 0) & (q < Q)

    def remote(src, dst, send, recv, to):
        return pltpu.make_async_remote_copy(
            src_ref=src, dst_ref=dst, send_sem=send, recv_sem=recv, device_id=to, device_id_type=MESH
        )

    def to_partner(q):
        return remote(grad.at[q % RING, 1 - c], pin.at[q % RING], p_send.at[q % SENDS], p_recv.at[q % RING], partner)

    def sum_right(q, frm):
        part = pl.ds(frm + 1, 3 - frm)
        return remote(rout.at[q % SENDS, part], rin.at[q % RING, part], r_send.at[q % SENDS], r_recv.at[q % RING], right)

    def sum_left(q, frm):
        part = pl.ds(0, frm)
        return remote(lout.at[q % SENDS, part], lin.at[q % RING, part], l_send.at[q % SENDS], l_recv.at[q % RING], left)

    def new_right(q, frm):
        part = pl.ds(0, frm + 1)
        here = wtmp.at[q, c, part]
        return remote(here, here, ar_send.at[q % SENDS], ar_recv.at[q % RING], right)

    def new_left(q, frm):
        part = pl.ds(frm, 4 - frm)
        here = wtmp.at[q, c, part]
        return remote(here, here, al_send.at[q % SENDS], al_recv.at[q % RING], left)

    def new_partner(q, core):
        here = wtmp.at[q, core]
        return remote(here, here, ap_send.at[q % SENDS], ap_recv.at[q % RING], partner)

    def keep_new(q):
        return pltpu.make_async_copy(wown.at[q % SENDS], wtmp.at[q, c, z], wo_sem.at[q % SENDS])

    def keep_grad(q):
        return pltpu.make_async_copy(gownb.at[q % SENDS], gown.at[q], go_sem.at[q % SENDS])

    def moments(q, act):
        layer = jnp.where(q < PER_LAYER, 1, 0)
        n = q % PER_LAYER
        s = q % 2
        cols = pl.ds(pl.multiple_of((n // 2) * CF, CF), CF)
        for which, (m, v, w) in enumerate(((mg, vg, wg), (mu, vu, wu))):

            @pl.when((n < 18) & (n % 2 == which))
            def _():
                own = pl.ds(pl.multiple_of(me * 112, 16), 112)
                act(pltpu.make_async_copy(m.at[layer, :, cols], mb.at[s], ad_sem.at[s, 0]))
                act(pltpu.make_async_copy(v.at[layer, :, cols], vb.at[s], ad_sem.at[s, 1]))
                act(pltpu.make_async_copy(w.at[layer, own, cols], wb.at[s], ad_sem.at[s, 2]))

        @pl.when(n >= 18)
        def _():
            rows = pl.ds(pl.multiple_of((n - 18) * 32, 32), 32)
            own = pl.ds(pl.multiple_of(me * 288 + (n - 18) * 32, 32), 32)
            act(pltpu.make_async_copy(md.at[layer, rows, :], mbd.at[s], ad_sem.at[s, 0]))
            act(pltpu.make_async_copy(vd.at[layer, rows, :], vbd.at[s], ad_sem.at[s, 1]))
            act(pltpu.make_async_copy(wd.at[layer, own, :], wbd.at[s], ad_sem.at[s, 2]))

    def new_weight(w, m, v, g):
        m = 0.9 * m + 0.1 * g
        v = 0.95 * v + 0.05 * g * g
        step = m * lax.rsqrt(v + 1e-8) + 0.1 * w
        return (w - 0.02 * step).astype(BF16)

    def weights_of(n, act):
        s = n % 2
        cols = pl.ds(pl.multiple_of((n % STEPS) * CF, CF), CF)
        layer = jnp.where((n >= STEPS) & (n < 2 * STEPS), 1, 0)

        @pl.when(n < 2 * STEPS)
        def _():
            act(pltpu.make_async_copy(wg.at[layer, :, cols], wgj.at[s], w_sem.at[s, 0]))
            act(pltpu.make_async_copy(wu.at[layer, :, cols], wuj.at[s], w_sem.at[s, 1]))

        @pl.when(n < 3 * STEPS)
        def _():
            act(pltpu.make_async_copy(wd.at[layer, cols, :], wdj.at[s], w_sem.at[s, 2]))

    def saved_of(j, act):
        @pl.when(j < STEPS)
        def _():
            act(pltpu.make_async_copy(g0.at[j], gbuf, gu_sem.at[0]))
            act(pltpu.make_async_copy(u0.at[j], ubuf, gu_sem.at[1]))

    def keep_saved(j, r):
        rows = pl.ds(pl.multiple_of(r * RB, RB), RB)
        return (
            pltpu.make_async_copy(gbuf.at[rows], g0.at[j, rows], keep_sem.at[r, 0]),
            pltpu.make_async_copy(ubuf.at[rows], u0.at[j, rows], keep_sem.at[r, 1]),
        )

    def keep_hidden0(j):
        return pltpu.make_async_copy(hid_c.at[j % 2], hid0_t.at[pl.ds(j * 8, 8)], hc_sem.at[j % 2])

    def keep_hidden(j):
        return pltpu.make_async_copy(hid_b, hid1_t.at[pl.ds(j * 8, 8)], hw_sem)

    def keep_d(j):
        cols = pl.ds(pl.multiple_of(j * CF, CF), CF)
        return (
            pltpu.make_async_copy(dg, dg1.at[:, cols], d_sem.at[0]),
            pltpu.make_async_copy(du, du1.at[:, cols], d_sem.at[1]),
        )

    def hidden_of(src, k, start):
        s = k % 2
        if start:
            for o in range(8):
                pltpu.make_async_copy(src.at[o * 9 + k], hid_c.at[s, o], hc_sem.at[s]).start()
        else:
            pltpu.make_async_copy(src.at[pl.ds(0, 8)], hid_c.at[s], hc_sem.at[s]).wait()

    load_x = pltpu.make_async_copy(x, xv, load_sem.at[0])
    load_dy = pltpu.make_async_copy(dy, dyv, load_sem.at[1])
    keep_at = pltpu.make_async_copy(at, a0_t, load_sem.at[2])
    load_at = pltpu.make_async_copy(a0_t, at, load_sem.at[2])

    start = lambda copy: copy.start()
    wait = lambda copy: copy.wait()

    def grad_columns(q, d):
        out = nn(at[...], d[...]).astype(BF16)
        for o in range(8):
            for h in range(2):
                grad[q % RING, o % 2, o // 2, h * 112 : (h + 1) * 112, :] = out[
                    o * 112 : (o + 1) * 112, h * 128 : (h + 1) * 128
                ]

    def grad_rows(q, k, d):
        out = nn(hid_c[k % 2].reshape(256, T), d[...]).astype(BF16)
        for o in range(8):
            for h in range(7):
                grad[q % RING, o % 2, o // 2, h * 32 : (h + 1) * 32, :] = out[
                    o * 32 : (o + 1) * 32, h * 128 : (h + 1) * 128
                ]

    def hidden_back(g, u, dp):
        s = sigmoid(g)
        act = g * s
        return act, (dp * u * (s + act * (1.0 - s))).astype(BF16), (dp * act).astype(BF16)

    def rows_of(r, n=RB):
        return pl.ds(pl.multiple_of(r * n, n), n)

    def forward(acc):
        weights_of(0, start)
        load_x.start()
        load_dy.start()
        load_x.wait()

        @pl.loop(0, NRB)
        def _(r):
            rows = rows_of(r)
            wide = xv[rows, :].astype(F32)
            a = (wide * norm_scale(wide)).astype(BF16)
            av[rows, :] = a
            at[:, rows] = a.T
            acc[rows, :] = jnp.zeros((RB, D), F32)

        keep_at.start()

        @pl.loop(0, STEPS)
        def _(j):
            b = j % 2
            weights_of(j + 1, start)
            weights_of(j, wait)

            @pl.when(j > 1)
            def _():
                keep_hidden0(j - 2).wait()

            @pl.loop(0, NRB)
            def _(r):
                rows = rows_of(r)

                @pl.when(j > 0)
                def _():
                    for copy in keep_saved(j - 1, r):
                        copy.wait()

                a = av[rows, :]
                g = nn(a, wgj[b])
                u = nn(a, wuj[b])
                gbuf[rows, :] = g
                ubuf[rows, :] = u
                hid = (g * sigmoid(g) * u).astype(BF16)
                hid_c[b, :, :, rows] = hid.T.reshape(8, 32, RB)
                acc[rows, :] += nn(hid, wdj[b])
                for copy in keep_saved(j, r):
                    copy.start()

            keep_hidden0(j).start()

        keep_at.wait()

        @pl.loop(0, NRB)
        def _(r):
            rows = rows_of(r)
            y = acc[rows, :].astype(BF16).astype(F32)
            h = (xv[rows, :].astype(F32) + y).astype(BF16)
            xv[rows, :] = h
            wide = h.astype(F32)
            a = (wide * norm_scale(wide)).astype(BF16)
            av[rows, :] = a
            at[:, rows] = a.T
            for copy in keep_saved(STEPS - 1, r):
                copy.wait()

        keep_hidden0(STEPS - 2).wait()
        keep_hidden0(STEPS - 1).wait()
        load_dy.wait()

    def first_layer(s):
        @pl.when(s % 2 == 0)
        def _():
            j = s // 2
            b = (j + 1) % 2
            weights_of(STEPS + j + 1, start)
            weights_of(STEPS + j, wait)

            @pl.when(j > 0)
            def _():
                keep_hidden(j - 1).wait()
                for copy in keep_d(j - 1):
                    copy.wait()

            @pl.loop(0, NRB)
            def _(r):
                rows = rows_of(r)
                a = av[rows, :]
                g = nn(a, wgj[b])
                u = nn(a, wuj[b])
                dp = nt(dyv[rows, :], wdj[b]).astype(BF16).astype(F32)
                act, dgr, dur = hidden_back(g, u, dp)
                hid_b[:, :, rows] = (act * u).astype(BF16).T.reshape(8, 32, RB)
                dg[rows, :] = dgr
                du[rows, :] = dur

            keep_hidden(j).start()
            for copy in keep_d(j):
                copy.start()
            grad_columns(s, dg)

        @pl.when(s % 2 == 1)
        def _():
            grad_columns(s, du)

            @pl.when(s == 17)
            def _():
                keep_hidden(STEPS - 1).wait()
                for copy in keep_d(STEPS - 1):
                    copy.wait()
                hidden_of(hid1_t, 0, True)
                load_at.start()
                saved_of(0, start)

    def between(s, wgl, wul, dgb, dub):
        k = s - 18
        block = lambda i: (
            pltpu.make_async_copy(dg1.at[rows_of(i, 256)], dgb, da_sem.at[2]),
            pltpu.make_async_copy(du1.at[rows_of(i, 256)], dub, da_sem.at[3]),
        )
        weights = (
            pltpu.make_async_copy(wg.at[1], wgl, da_sem.at[0]),
            pltpu.make_async_copy(wu.at[1], wul, da_sem.at[1]),
        )

        @pl.when(k == 0)
        def _():
            for copy in (*weights, *block(0)):
                copy.start()

        @pl.when(k < 8)
        def _():
            hidden_of(hid1_t, k + 1, True)

        hidden_of(hid1_t, k, False)
        grad_rows(s, k, dyv)

        @pl.when(k == 1)
        def _():
            for copy in weights:
                copy.wait()

        @pl.when(k > 0)
        def _():
            for copy in block(k - 1):
                copy.wait()
            by_g = nt(dgb[...], wgl[...])
            by_u = nt(dub[...], wul[...])
            da = by_g.astype(BF16).astype(F32) + by_u.astype(BF16).astype(F32)
            da = da.astype(BF16).astype(F32)
            rows = rows_of(k - 1, 256)
            wide = xv[rows, :].astype(F32)
            scale = norm_scale(wide)
            along = jnp.sum(da * wide, -1, keepdims=True) * (scale * scale * scale) * (-1.0 / D)
            back = (da * scale + wide * along).astype(BF16)
            xv[rows, :] = (dyv[rows, :].astype(F32) + back.astype(F32)).astype(BF16)

            @pl.when(k < 8)
            def _():
                for copy in block(k):
                    copy.start()

        @pl.when(k == 8)
        def _():
            load_at.wait()

    def last_layer(s):
        @pl.when((s < 45) & ((s - 27) % 2 == 0))
        def _():
            j = (s - 27) // 2
            b = j % 2
            weights_of(2 * STEPS + j + 1, start)
            weights_of(2 * STEPS + j, wait)
            saved_of(j, wait)

            @pl.loop(0, NRB)
            def _(r):
                rows = rows_of(r)
                dp = nt(xv[rows, :], wdj[b]).astype(BF16).astype(F32)
                _, dgr, dur = hidden_back(gbuf[rows, :], ubuf[rows, :], dp)
                dg[rows, :] = dgr
                du[rows, :] = dur

            saved_of(j + 1, start)
            grad_columns(s, dg)

        @pl.when((s < 45) & ((s - 27) % 2 == 1))
        def _():
            grad_columns(s, du)

            @pl.when(s == 44)
            def _():
                hidden_of(hid0_t, 0, True)

        @pl.when((s >= 45) & (s < 54))
        def _():
            k = s - 45

            @pl.when(k < 8)
            def _():
                hidden_of(hid0_t, k + 1, True)

            hidden_of(hid0_t, k, False)
            grad_rows(s, k, xv)

    f32 = lambda t: t.astype(F32)

    def exchange(s):
        q = s - 1

        @pl.when(valid(q))
        def _():
            to_partner(q).wait_recv()

        qr = s - 1 - 2 * z
        for zz in range(4):

            @pl.when(valid(qr) & (z == zz))
            def _():
                if zz > 0:
                    sum_right(qr, zz - 1).wait_recv()
                if zz < 3:

                    @pl.when(qr >= SENDS)
                    def _():
                        sum_right(qr - SENDS, zz).wait_send()

                    e = qr % RING
                    for to in range(zz + 1, 4):
                        t = f32(grad[e, c, to]) + f32(pin[e, to])
                        if zz > 0:
                            t = t + f32(rin[e, to])
                        rout[qr % SENDS, to] = t.astype(BF16)
                    sum_right(qr, zz).start()

        ql = s - 1 - 2 * (3 - z)
        for zz in range(4):

            @pl.when(valid(ql) & (z == zz))
            def _():
                if zz < 3:
                    sum_left(ql, zz + 1).wait_recv()
                if zz > 0:

                    @pl.when(ql >= SENDS)
                    def _():
                        sum_left(ql - SENDS, zz).wait_send()

                    e = ql % RING
                    for to in range(zz):
                        t = f32(grad[e, c, to]) + f32(pin[e, to])
                        if zz < 3:
                            t = t + f32(lin[e, to])
                        lout[ql % SENDS, to] = t.astype(BF16)
                    sum_left(ql, zz).start()

        for zz in range(4):

            @pl.when((qr >= Q) & (qr < Q + SENDS) & (z == zz))
            def _():
                if zz < 3:
                    sum_right(qr - SENDS, zz).wait_send()

            @pl.when((ql >= Q) & (ql < Q + SENDS) & (z == zz))
            def _():
                if zz > 0:
                    sum_left(ql - SENDS, zz).wait_send()

        @pl.when(valid(s - 6))
        def _():
            moments(s - 6, start)

        qf = s - 7

        @pl.when((qf >= SENDS) & (qf < Q + SENDS))
        def _():
            keep_grad(qf - SENDS).wait()

        @pl.when(valid(qf))
        def _():
            e, b = qf % RING, qf % SENDS
            gfin[...] = f32(grad[e, c, z]) + f32(pin[e, z])

            @pl.when(z > 0)
            def _():
                gfin[...] += f32(rin[e, z])

            @pl.when(z < 3)
            def _():
                gfin[...] += f32(lin[e, z])

            gownb[b] = gfin[...].astype(BF16)
            keep_grad(qf).start()
            moments(qf, wait)
            n = qf % PER_LAYER
            sl = qf % 2

            @pl.when(n < 18)
            def _():
                for h in range(2):
                    lanes = slice(h * 128, (h + 1) * 128)
                    part = slice(h * 112, (h + 1) * 112)
                    g = gownb[b, part, :].astype(F32)
                    wown[b, part, :] = new_weight(f32(wb[sl, :, lanes]), mb[sl, :, lanes], vb[sl, :, lanes], g)

            @pl.when(n >= 18)
            def _():
                for h in range(7):
                    lanes = slice(h * 128, (h + 1) * 128)
                    part = slice(h * 32, (h + 1) * 32)
                    g = gownb[b, part, :].astype(F32)
                    wown[b, part, :] = new_weight(f32(wbd[sl, :, lanes]), mbd[sl, :, lanes], vbd[sl, :, lanes], g)

            keep_new(qf).start()

        @pl.when(valid(s - 8))
        def _():
            keep_new(s - 8).wait()

        qar = s - 8 - 2 * z
        qal = s - 8 - 2 * (3 - z)
        for zz in range(4):

            @pl.when(valid(qar) & (z == zz))
            def _():
                if zz > 0:
                    new_right(qar, zz - 1).wait_recv()
                if zz < 3:

                    @pl.when(qar >= SENDS)
                    def _():
                        new_right(qar - SENDS, zz).wait_send()

                    new_right(qar, zz).start()

            @pl.when(valid(qal) & (z == zz))
            def _():
                if zz < 3:
                    new_left(qal, zz + 1).wait_recv()
                if zz > 0:

                    @pl.when(qal >= SENDS)
                    def _():
                        new_left(qal - SENDS, zz).wait_send()

                    new_left(qal, zz).start()

            @pl.when((qar >= Q) & (qar < Q + SENDS) & (z == zz))
            def _():
                if zz < 3:
                    new_right(qar - SENDS, zz).wait_send()

            @pl.when((qal >= Q) & (qal < Q + SENDS) & (z == zz))
            def _():
                if zz > 0:
                    new_left(qal - SENDS, zz).wait_send()

        qap = s - 14

        @pl.when((qap >= SENDS) & (qap < Q + SENDS))
        def _():
            new_partner(qap - SENDS, c).wait_send()

        @pl.when(valid(qap))
        def _():
            new_partner(qap, c).start()

        @pl.when(valid(s - 16))
        def _():
            new_partner(s - 16, 1 - c).wait_recv()

    def slots(first, last, compute):
        @pl.loop(first, last)
        def _(s):
            @pl.when(s < Q)
            def _():
                compute(s)

            @pl.when((s >= SENDS) & (s < Q + SENDS))
            def _():
                to_partner(s - SENDS).wait_send()

            @pl.when(s < Q)
            def _():
                to_partner(s).start()

            exchange(s)

    pl.run_scoped(forward, pltpu.VMEM((T, D), F32))
    slots(0, 18, first_layer)
    pl.run_scoped(
        lambda *bufs: slots(18, 27, lambda s: between(s, *bufs)),
        pltpu.VMEM((D, FF), BF16), pltpu.VMEM((D, FF), BF16), pltpu.VMEM((256, FF), BF16), pltpu.VMEM((256, FF), BF16),
    )
    slots(27, LAST, last_layer)


def train(*operands):
    vm = pltpu.VMEM
    dma = pltpu.SemaphoreType.DMA
    any_ = pl.BlockSpec(memory_space=pl.ANY)
    shape = jax.ShapeDtypeStruct
    out_shape = [
        shape((Q, 2, 4, ROWS, 128), BF16), shape((Q, ROWS, 128), BF16),
        shape((72, 32, T), BF16), shape((72, 32, T), BF16), shape((D, T), BF16),
        shape((STEPS, T, CF), F32), shape((STEPS, T, CF), F32), shape((T, FF), BF16), shape((T, FF), BF16),
    ]
    return pl.pallas_call(
        train_kernel,
        in_specs=[any_] * len(operands),
        out_specs=[any_] * len(out_shape),
        out_shape=out_shape,
        scratch_shapes=[
            vm((T, D), BF16), vm((T, D), BF16), vm((T, D), BF16), vm((D, T), BF16),
            vm((T, CF), F32), vm((T, CF), F32), vm((T, CF), BF16), vm((T, CF), BF16),
            vm((2, D, CF), BF16), vm((2, D, CF), BF16), vm((2, CF, D), BF16),
            vm((8, 32, T), BF16), vm((2, 8, 32, T), BF16),
            vm((RING, 2, 4, ROWS, 128), BF16), vm((RING, 4, ROWS, 128), BF16),
            vm((RING, 4, ROWS, 128), BF16), vm((RING, 4, ROWS, 128), BF16),
            vm((SENDS, 4, ROWS, 128), BF16), vm((SENDS, 4, ROWS, 128), BF16),
            vm((SENDS, ROWS, 128), BF16), vm((SENDS, ROWS, 128), BF16), vm((ROWS, 128), F32),
            vm((2, 112, CF), F32), vm((2, 112, CF), F32), vm((2, 112, CF), BF16),
            vm((2, 32, D), F32), vm((2, 32, D), F32), vm((2, 32, D), BF16),
            dma((3,)), dma((2, 3)), dma((2,)), dma((NRB, 2)), dma, dma((2,)), dma((2,)), dma((4,)),
            dma((SENDS,)), dma((RING,)), dma((SENDS,)), dma((RING,)), dma((SENDS,)), dma((RING,)),
            dma((SENDS,)), dma((RING,)), dma((SENDS,)), dma((RING,)), dma((SENDS,)), dma((RING,)),
            dma((SENDS,)), dma((SENDS,)), dma((2, 3)),
        ],
        compiler_params=pltpu.CompilerParams(
            collective_id=0, has_side_effects=True, vmem_limit_bytes=VMEM_LIMIT
        ),
        name="train",
    )(*operands)


def finish_kernel(wt_g, wt_u, wt_d, gg, gu, gd, mg, mu, md, vg, vu, vd, owg, owu, owd, omg, omu, omd, ovg, ovu, ovd):
    for src, dst in ((wt_g, owg), (wt_u, owu)):
        for o in range(8):
            for h in range(2):
                dst[0, o * 112 : (o + 1) * 112, h * 128 : (h + 1) * 128] = src[0, o % 2, o // 2, h * 112 : (h + 1) * 112, :]
    for o in range(8):
        for h in range(7):
            owd[0, o, :, h * 128 : (h + 1) * 128] = wt_d[0, o % 2, o // 2, h * 32 : (h + 1) * 32, :]
    for g, m, v, om, ov, n, rows in ((gg, mg, vg, omg, ovg, 2, 112), (gu, mu, vu, omu, ovu, 2, 112), (gd, md, vd, omd, ovd, 7, 32)):
        for h in range(n):
            lanes = slice(h * 128, (h + 1) * 128)
            gr = g[0, h * rows : (h + 1) * rows, :].astype(F32)
            om[0, :, lanes] = 0.9 * m[0, :, lanes] + 0.1 * gr
            ov[0, :, lanes] = 0.95 * v[0, :, lanes] + 0.05 * gr * gr


def finish(wtmp, gown, m, v):
    layer = lambda i: i // STEPS
    first = lambda i: (1 - i // STEPS) * PER_LAYER
    chunk = (lambda i: first(i) + 2 * (i % STEPS), lambda i: first(i) + 2 * (i % STEPS) + 1, lambda i: first(i) + 18 + i % STEPS)
    blocks = [pl.BlockSpec((1, 2, 4, ROWS, 128), functools.partial(lambda f, i: (f(i), 0, 0, 0, 0), f)) for f in chunk]
    grads = [pl.BlockSpec((1, ROWS, 128), functools.partial(lambda f, i: (f(i), 0, 0), f)) for f in chunk]
    cols = pl.BlockSpec((1, 112, CF), lambda i: (layer(i), 0, i % STEPS))
    rows = pl.BlockSpec((1, 32, D), lambda i: (layer(i), i % STEPS, 0))
    wcols = pl.BlockSpec((1, D, CF), lambda i: (layer(i), 0, i % STEPS))
    wrows = pl.BlockSpec((1, 8, 32, D), lambda i: (layer(i), 0, i % STEPS, 0))
    out = pl.pallas_call(
        finish_kernel,
        grid=(2 * STEPS,),
        in_specs=[*blocks, *grads, cols, cols, rows, cols, cols, rows],
        out_specs=[wcols, wcols, wrows, cols, cols, rows, cols, cols, rows],
        out_shape=[
            jax.ShapeDtypeStruct((2, D, FF), BF16), jax.ShapeDtypeStruct((2, D, FF), BF16),
            jax.ShapeDtypeStruct((2, 8, 288, D), BF16),
            *[jax.ShapeDtypeStruct(t.shape, F32) for t in (*m, *v)],
        ],
        compiler_params=pltpu.CompilerParams(vmem_limit_bytes=VMEM_LIMIT, dimension_semantics=("arbitrary",)),
        name="finish",
    )(wtmp, wtmp, wtmp, gown, gown, gown, *m, *v)
    return (out[0], out[1], out[2].reshape(2, FF, D), *out[3:])


def solution(mesh):
    def step(x, dy, wg, wu, wd, *moments):
        m, v = moments[:3], moments[3:]
        wtmp, gown, *_ = train(wg, wu, wd, *m, *v, x[0], dy[0])
        return finish(wtmp, gown, m, v)

    seq, whole, rows = P(("rep", "dp")), P(), P(None, "dp")
    return jax.shard_map(
        step, mesh=mesh,
        in_specs=(seq, seq, *[whole] * 3, *[rows] * 6),
        out_specs=(*[P("rep")] * 3, *[P("rep", "dp")] * 6),
        check_vma=False,
    )
```

```python
import jax
import jax.numpy as jnp
from jax import lax
from jax.experimental import pallas as pl
from jax.experimental.pallas import tpu as pltpu
from jax.sharding import PartitionSpec as P

MESH = pl.DeviceIdType.MESH
F32, BF16 = jnp.float32, jnp.bfloat16
T, D, FF = 2048, 896, 2304
CF = 256
STEPS = FF // CF
RB = 1024
NRB = T // RB
ROWS = 112
PER_LAYER = 27
CHUNKS = 2 * PER_LAYER
Q = 2 * CHUNKS
LAG = 2
HELD = 8
RING = 2 * HELD
SENDS = 4
SPREAD = 4 + 6 * LAG
LAST = Q + SPREAD + 3
VMEM_LIMIT = 67043328


def nt(a, b):
    return lax.dot_general(a, b, (((1,), (1,)), ((), ())), preferred_element_type=F32)


def nn(a, b):
    return jnp.dot(a, b, preferred_element_type=F32)


def norm_scale(wide):
    return lax.rsqrt(jnp.mean(wide * wide, -1, keepdims=True) + 1e-6)


def sigmoid(g):
    return 1.0 / (1.0 + jnp.exp(-g))


def train_kernel(
    wg, wu, wd, mg, mu, md, vg, vu, vd, x, dy,
    wtmp, nmg, nmu, nmd, nvg, nvu, nvd, hid0_t, hid1_t, g0, u0, dg1, du1,
    xv, dyv, av, at, gbuf, ubuf, dg, du, wgj, wuj, wdj, hid_b, hid_c,
    grad, pin, rin, lin, rout, lout, news, gfin, mb, vb, wb, mbd, vbd, wbd,
    load_sem, w_sem, gu_sem, keep_sem, hw_sem, hc_sem, d_sem, da_sem,
    p_send, p_recv, r_send, r_recv, l_send, l_recv,
    or_send, or_recv, ol_send, ol_recv, ar_send, ar_recv, al_send, al_recv, ap_send, ap_recv, wo_sem, mo_sem, ad_sem,
):
    rep, me = lax.axis_index("rep"), lax.axis_index("dp")
    z, c = me // 2, me % 2
    partner = (rep, z * 2 + (1 - c))
    right = (rep, jnp.minimum(z + 1, 3) * 2 + c)
    left = (rep, jnp.maximum(z - 1, 0) * 2 + c)

    bar = pltpu.get_barrier_semaphore()
    pl.semaphore_signal(bar, inc=1, device_id=partner, device_id_type=MESH)

    @pl.when(z < 3)
    def _():
        pl.semaphore_signal(bar, inc=1, device_id=right, device_id_type=MESH)

    @pl.when(z > 0)
    def _():
        pl.semaphore_signal(bar, inc=1, device_id=left, device_id_type=MESH)

    valid = lambda q: (q >= 0) & (q < Q)

    def remote(src, dst, send, recv, to):
        return pltpu.make_async_remote_copy(
            src_ref=src, dst_ref=dst, send_sem=send, recv_sem=recv, device_id=to, device_id_type=MESH
        )

    def to_partner(p):
        e = p % HELD
        return remote(grad.at[e, 1 - c], pin.at[e], p_send.at[p % 2], p_recv.at[e], partner)

    def sum_right(q, frm):
        part = pl.ds(frm + 1, 3 - frm)
        return remote(rout.at[q % SENDS, part], rin.at[q % RING, part], r_send.at[q % SENDS], r_recv.at[q % RING], right)

    def sum_left(q, frm):
        part = pl.ds(0, frm)
        return remote(lout.at[q % SENDS, part], lin.at[q % RING, part], l_send.at[q % SENDS], l_recv.at[q % RING], left)

    def own_right(q, frm):
        here = news.at[q % RING, pl.ds(frm, 1)]
        return remote(here, here, or_send.at[q % SENDS], or_recv.at[q % RING], right)

    def own_left(q, frm):
        here = news.at[q % RING, pl.ds(frm, 1)]
        return remote(here, here, ol_send.at[q % SENDS], ol_recv.at[q % RING], left)

    def on_right(q, frm):
        here = news.at[q % RING, pl.ds(0, frm)]
        return remote(here, here, ar_send.at[q % SENDS], ar_recv.at[q % RING], right)

    def on_left(q, frm):
        here = news.at[q % RING, pl.ds(frm + 1, 3 - frm)]
        return remote(here, here, al_send.at[q % SENDS], al_recv.at[q % RING], left)

    def new_partner(q, core):
        return remote(
            news.at[q % RING], wtmp.at[q // 2, core, q % 2], ap_send.at[q % SENDS], ap_recv.at[q % RING], partner
        )

    def keep_new(q):
        return pltpu.make_async_copy(news.at[q % RING], wtmp.at[q // 2, c, q % 2], wo_sem.at[q % SENDS])

    def moments(q, act, new=False):
        p = q // 2
        layer = jnp.where(p < PER_LAYER, 1, 0)
        n = p % PER_LAYER
        s = q % 2
        cols = pl.ds(pl.multiple_of((n // 2) * CF + s * 128, 128), 128)
        for which, (m, v, w, nm, nv) in enumerate(((mg, vg, wg, nmg, nvg), (mu, vu, wu, nmu, nvu))):

            @pl.when((n < 18) & (n % 2 == which))
            def _():
                if new:
                    act(pltpu.make_async_copy(mb.at[s], nm.at[layer, :, cols], mo_sem.at[s, 0]))
                    act(pltpu.make_async_copy(vb.at[s], nv.at[layer, :, cols], mo_sem.at[s, 1]))
                else:
                    own = pl.ds(pl.multiple_of(me * 112, 16), 112)
                    act(pltpu.make_async_copy(m.at[layer, :, cols], mb.at[s], ad_sem.at[s, 0]))
                    act(pltpu.make_async_copy(v.at[layer, :, cols], vb.at[s], ad_sem.at[s, 1]))
                    act(pltpu.make_async_copy(w.at[layer, own, cols], wb.at[s], ad_sem.at[s, 2]))

        @pl.when(n >= 18)
        def _():
            rows = pl.ds(pl.multiple_of((n - 18) * 32 + s * 16, 16), 16)
            if new:
                act(pltpu.make_async_copy(mbd.at[s], nmd.at[layer, rows, :], mo_sem.at[s, 0]))
                act(pltpu.make_async_copy(vbd.at[s], nvd.at[layer, rows, :], mo_sem.at[s, 1]))
            else:
                own = pl.ds(pl.multiple_of(me * 288 + (n - 18) * 32 + s * 16, 16), 16)
                act(pltpu.make_async_copy(md.at[layer, rows, :], mbd.at[s], ad_sem.at[s, 0]))
                act(pltpu.make_async_copy(vd.at[layer, rows, :], vbd.at[s], ad_sem.at[s, 1]))
                act(pltpu.make_async_copy(wd.at[layer, own, :], wbd.at[s], ad_sem.at[s, 2]))

    def adamw(w, m, v, g):
        m = 0.9 * m + 0.1 * g
        v = 0.95 * v + 0.05 * g * g
        step = m * lax.rsqrt(v + 1e-8) + 0.1 * w
        return (w - 0.02 * step).astype(BF16), m, v

    def weights_of(n, act):
        s = n % 2
        cols = pl.ds(pl.multiple_of((n % STEPS) * CF, CF), CF)
        layer = jnp.where((n >= STEPS) & (n < 2 * STEPS), 1, 0)

        @pl.when(n < 2 * STEPS)
        def _():
            act(pltpu.make_async_copy(wg.at[layer, :, cols], wgj.at[s], w_sem.at[s, 0]))
            act(pltpu.make_async_copy(wu.at[layer, :, cols], wuj.at[s], w_sem.at[s, 1]))

        @pl.when(n < 3 * STEPS)
        def _():
            act(pltpu.make_async_copy(wd.at[layer, cols, :], wdj.at[s], w_sem.at[s, 2]))

    def saved_of(j, act):
        @pl.when(j < STEPS)
        def _():
            act(pltpu.make_async_copy(g0.at[j], gbuf, gu_sem.at[0]))
            act(pltpu.make_async_copy(u0.at[j], ubuf, gu_sem.at[1]))

    def keep_saved(j, r):
        rows = pl.ds(pl.multiple_of(r * RB, RB), RB)
        return (
            pltpu.make_async_copy(gbuf.at[rows], g0.at[j, rows], keep_sem.at[r, 0]),
            pltpu.make_async_copy(ubuf.at[rows], u0.at[j, rows], keep_sem.at[r, 1]),
        )

    def keep_hidden0(j):
        return pltpu.make_async_copy(hid_c.at[j % 2], hid0_t.at[pl.ds(j * 8, 8)], hc_sem.at[j % 2])

    def keep_hidden(j):
        return pltpu.make_async_copy(hid_b, hid1_t.at[pl.ds(j * 8, 8)], hw_sem)

    def keep_d(j):
        cols = pl.ds(pl.multiple_of(j * CF, CF), CF)
        return (
            pltpu.make_async_copy(dg, dg1.at[:, cols], d_sem.at[0]),
            pltpu.make_async_copy(du, du1.at[:, cols], d_sem.at[1]),
        )

    def hidden_of(src, k, start):
        s = k % 2
        if start:
            for o in range(8):
                pltpu.make_async_copy(src.at[o * 9 + k], hid_c.at[s, o], hc_sem.at[s]).start()
        else:
            pltpu.make_async_copy(src.at[pl.ds(0, 8)], hid_c.at[s], hc_sem.at[s]).wait()

    load_dy = pltpu.make_async_copy(dy, dyv, load_sem.at[2])

    start = lambda copy: copy.start()
    wait = lambda copy: copy.wait()

    def grad_columns(p, d):
        out = nn(at[...], d[...]).astype(BF16)
        for o in range(8):
            for h in range(2):
                grad[p % HELD, o % 2, h, o // 2] = out[o * 112 : (o + 1) * 112, h * 128 : (h + 1) * 128]

    def grad_rows(p, k, d):
        out = nn(hid_c[k % 2].reshape(256, T), d[...]).astype(BF16)
        for o in range(8):
            for h in range(2):
                for i in range(7):
                    grad[p % HELD, o % 2, h, o // 2, i * 16 : (i + 1) * 16, :] = out[
                        o * 32 + h * 16 : o * 32 + h * 16 + 16, i * 128 : (i + 1) * 128
                    ]

    def hidden_back(g, u, dp):
        s = sigmoid(g)
        act = g * s
        return act, (dp * u * (s + act * (1.0 - s))).astype(BF16), (dp * act).astype(BF16)

    def rows_of(r, n=RB):
        return pl.ds(pl.multiple_of(r * n, n), n)

    def forward(acc):
        weights_of(0, start)
        halves = [pltpu.make_async_copy(x.at[rows_of(r)], xv.at[rows_of(r)], load_sem.at[r]) for r in range(NRB)]
        for copy in halves:
            copy.start()
        load_dy.start()
        for r in range(NRB):
            halves[r].wait()
            rows = rows_of(r)
            wide = xv[rows, :].astype(F32)
            av[rows, :] = (wide * norm_scale(wide)).astype(BF16)

        @pl.loop(0, NRB * STEPS)
        def _(i):
            j, r = i // NRB, i % NRB
            b = j % 2
            rows = rows_of(r)

            @pl.when(r == 0)
            def _():
                weights_of(j + 1, start)
                weights_of(j, wait)

                @pl.when(j > 1)
                def _():
                    keep_hidden0(j - 2).wait()

            @pl.when(j > 0)
            def _():
                for copy in keep_saved(j - 1, r):
                    copy.wait()

            a = av[rows, :]
            g = nn(a, wgj[b])
            u = nn(a, wuj[b])
            gbuf[rows, :] = g
            ubuf[rows, :] = u
            hid = (g * sigmoid(g) * u).astype(BF16)
            hid_c[b, :, :, rows] = hid.T.reshape(8, 32, RB)
            acc[rows, :] = jnp.where(j == 0, 0.0, acc[rows, :]) + nn(hid, wdj[b])
            for copy in keep_saved(j, r):
                copy.start()

            @pl.when(r == NRB - 1)
            def _():
                keep_hidden0(j).start()

        @pl.loop(0, NRB)
        def _(r):
            rows = rows_of(r)
            y = acc[rows, :].astype(BF16).astype(F32)
            h = (xv[rows, :].astype(F32) + y).astype(BF16)
            xv[rows, :] = h
            wide = h.astype(F32)
            a = (wide * norm_scale(wide)).astype(BF16)
            av[rows, :] = a
            at[:, rows] = a.T
            for copy in keep_saved(STEPS - 1, r):
                copy.wait()

        keep_hidden0(STEPS - 2).wait()
        keep_hidden0(STEPS - 1).wait()
        load_dy.wait()

    def first_layer(t):
        j = t // 4
        b = (j + 1) % 2

        @pl.when(t % 4 == 0)
        def _():
            weights_of(STEPS + j + 1, start)
            weights_of(STEPS + j, wait)

            @pl.when(j > 0)
            def _():
                keep_hidden(j - 1).wait()
                for copy in keep_d(j - 1):
                    copy.wait()

        @pl.when(t % 4 < 2)
        def _():
            rows = rows_of(t % 4)
            a = av[rows, :]
            g = nn(a, wgj[b])
            u = nn(a, wuj[b])
            dp = nt(dyv[rows, :], wdj[b]).astype(BF16).astype(F32)
            act, dgr, dur = hidden_back(g, u, dp)
            hid_b[:, :, rows] = (act * u).astype(BF16).T.reshape(8, 32, RB)
            dg[rows, :] = dgr
            du[rows, :] = dur

        @pl.when(t % 4 == 2)
        def _():
            keep_hidden(j).start()
            for copy in keep_d(j):
                copy.start()
            grad_columns(2 * j, dg)

        @pl.when(t % 4 == 3)
        def _():
            grad_columns(2 * j + 1, du)

            @pl.when(j == STEPS - 1)
            def _():
                keep_hidden(STEPS - 1).wait()
                for copy in keep_d(STEPS - 1):
                    copy.wait()
                hidden_of(hid1_t, 0, True)
                saved_of(0, start)

    def between(t, wgl, wul, dgb, dub, xb):
        k = (t - 36) // 2
        block = lambda i: (
            pltpu.make_async_copy(dg1.at[rows_of(i, 256)], dgb, da_sem.at[2]),
            pltpu.make_async_copy(du1.at[rows_of(i, 256)], dub, da_sem.at[3]),
            pltpu.make_async_copy(x.at[rows_of(i, 256)], xb, da_sem.at[4]),
        )
        weights = (
            pltpu.make_async_copy(wg.at[1], wgl, da_sem.at[0]),
            pltpu.make_async_copy(wu.at[1], wul, da_sem.at[1]),
        )

        @pl.when(t == 36)
        def _():
            for copy in (*weights, *block(0)):
                copy.start()

        @pl.when(t == 38)
        def _():
            for copy in weights:
                copy.wait()

        @pl.when((k > 0) & (t % 2 == 0))
        def _():
            for copy in block(k - 1):
                copy.wait()
            by_g = nt(dgb[...], wgl[...])
            by_u = nt(dub[...], wul[...])
            da = by_g.astype(BF16).astype(F32) + by_u.astype(BF16).astype(F32)
            da = da.astype(BF16).astype(F32)
            rows = rows_of(k - 1, 256)
            wide = xv[rows, :].astype(F32)
            scale = norm_scale(wide)
            along = jnp.sum(da * wide, -1, keepdims=True) * (scale * scale * scale) * (-1.0 / D)
            back = (da * scale + wide * along).astype(BF16)
            xv[rows, :] = (dyv[rows, :].astype(F32) + back.astype(F32)).astype(BF16)
            wide = xb[...].astype(F32)
            at[:, rows] = (wide * norm_scale(wide)).astype(BF16).T

            @pl.when(k < 8)
            def _():
                for copy in block(k):
                    copy.start()

        @pl.when(t % 2 == 1)
        def _():
            @pl.when(k < 8)
            def _():
                hidden_of(hid1_t, k + 1, True)

            hidden_of(hid1_t, k, False)
            grad_rows(18 + k, k, dyv)

    def last_layer(t):
        j = (t - 54) // 4
        b = j % 2
        turn = (t - 54) % 4
        k = (t - 90) // 2

        @pl.when((t < 90) & (turn == 0))
        def _():
            weights_of(2 * STEPS + j + 1, start)
            weights_of(2 * STEPS + j, wait)
            saved_of(j, wait)

        @pl.when((t < 90) & (turn < 2))
        def _():
            rows = rows_of(turn)
            dp = nt(xv[rows, :], wdj[b]).astype(BF16).astype(F32)
            _, dgr, dur = hidden_back(gbuf[rows, :], ubuf[rows, :], dp)
            dg[rows, :] = dgr
            du[rows, :] = dur

        @pl.when((t < 90) & (turn == 2))
        def _():
            saved_of(j + 1, start)
            grad_columns(PER_LAYER + 2 * j, dg)

        @pl.when((t < 90) & (turn == 3))
        def _():
            grad_columns(PER_LAYER + 2 * j + 1, du)

            @pl.when(t == 89)
            def _():
                hidden_of(hid0_t, 0, True)

        @pl.when((t >= 90) & (t < Q) & (t % 2 == 1))
        def _():
            @pl.when(k < 8)
            def _():
                hidden_of(hid0_t, k + 1, True)

            hidden_of(hid0_t, k, False)
            grad_rows(PER_LAYER + 18 + k, k, xv)

    def chunk_after(t):
        n = t % 54
        pair = n < 36
        return (t < Q) & jnp.where(pair, n % 4 >= 2, n % 2 == 1), (t // 54) * PER_LAYER + jnp.where(
            pair, 2 * (n // 4) + n % 2, n // 2
        )

    f32 = lambda t: t.astype(F32)

    def sums(t):
        q = t - 3

        @pl.when(valid(q) & (q % 2 == 0))
        def _():
            to_partner(q // 2).wait_recv()

        qr = t - 3 - LAG * z
        ql = t - 3 - LAG * (3 - z)

        def own(q, to):
            e = (q // 2) % HELD
            return f32(grad[e, c, q % 2, to]) + f32(pin[e, q % 2, to])

        for zz in range(4):

            @pl.when(z == zz)
            def _():
                @pl.when(valid(qr))
                def _():
                    if zz > 0:
                        sum_right(qr, zz - 1).wait_recv()
                    if zz < 3:

                        @pl.when(qr >= SENDS)
                        def _():
                            sum_right(qr - SENDS, zz).wait_send()

                        for to in range(zz + 1, 4):
                            total = own(qr, to)
                            if zz > 0:
                                total = total + f32(rin[qr % RING, to])
                            rout[qr % SENDS, to] = total.astype(BF16)
                        sum_right(qr, zz).start()

                @pl.when(valid(ql))
                def _():
                    if zz < 3:
                        sum_left(ql, zz + 1).wait_recv()
                    if zz > 0:

                        @pl.when(ql >= SENDS)
                        def _():
                            sum_left(ql - SENDS, zz).wait_send()

                        for to in range(zz):
                            total = own(ql, to)
                            if zz < 3:
                                total = total + f32(lin[ql % RING, to])
                            lout[ql % SENDS, to] = total.astype(BF16)
                        sum_left(ql, zz).start()

    def optimizer(t):
        q = t - 3 - LAG * jnp.maximum(z, 3 - z)

        @pl.when((q >= 1) & (q <= Q))
        def _():
            moments(q - 1, wait, new=True)

        @pl.when(valid(q + 1))
        def _():
            moments(q + 1, start)

        @pl.when(valid(q))
        def _():
            e, h = (q // 2) % HELD, q % 2
            gfin[...] = f32(grad[e, c, h, z]) + f32(pin[e, h, z])

            @pl.when(z > 0)
            def _():
                gfin[...] += f32(rin[q % RING, z])

            @pl.when(z < 3)
            def _():
                gfin[...] += f32(lin[q % RING, z])

            moments(q, wait)
            n = (q // 2) % PER_LAYER

            @pl.when(n < 18)
            def _():
                g = f32(gfin[...].astype(BF16))
                news[q % RING, z], mb[h], vb[h] = adamw(f32(wb[h]), mb[h], vb[h], g)

            @pl.when(n >= 18)
            def _():
                for i in range(7):
                    lanes = slice(i * 128, (i + 1) * 128)
                    part = slice(i * 16, (i + 1) * 16)
                    g = f32(gfin[part, :].astype(BF16))
                    news[q % RING, z, part, :], mbd[h, :, lanes], vbd[h, :, lanes] = adamw(
                        f32(wbd[h, :, lanes]), mbd[h, :, lanes], vbd[h, :, lanes], g
                    )

            moments(q, start, new=True)

    def send(copy, q, frm):
        @pl.when(q >= SENDS)
        def _():
            copy(q - SENDS, frm).wait_send()

        copy(q, frm).start()

    def spread(t):
        for zz in range(4):

            @pl.when(z == zz)
            def _():
                q = t - 4 - LAG * max(zz, 3 - zz)

                @pl.when(valid(q))
                def _():
                    if zz < 3:
                        send(own_right, q, zz)
                    if zz > 0:
                        send(own_left, q, zz)

                if zz in (1, 2):
                    near, far = t - 4 - 4 * LAG, t - 4 - 5 * LAG
                    qr, ql = (near, far) if zz == 1 else (far, near)

                    @pl.when(valid(qr))
                    def _():
                        own_right(qr, zz - 1).wait_recv()
                        if zz == 2:
                            on_right(qr, 1).wait_recv()
                        send(on_right, qr, zz)

                    @pl.when(valid(ql))
                    def _():
                        own_left(ql, zz + 1).wait_recv()
                        if zz == 1:
                            on_left(ql, 2).wait_recv()
                        send(on_left, ql, zz)
                else:
                    q = t - SPREAD

                    @pl.when(valid(q))
                    def _():
                        if zz == 3:
                            own_right(q, 2).wait_recv()
                            on_right(q, 2).wait_recv()
                        else:
                            own_left(q, 1).wait_recv()
                            on_left(q, 1).wait_recv()

        q = t - SPREAD

        @pl.when(valid(q))
        def _():
            @pl.when(q >= SENDS)
            def _():
                new_partner(q - SENDS, c).wait_send()
                keep_new(q - SENDS).wait()

            new_partner(q, c).start()
            keep_new(q).start()

        @pl.when(valid(q - 2))
        def _():
            new_partner(q - 2, 1 - c).wait_recv()

    def last_waits():
        for i in range(2):
            to_partner(CHUNKS - 2 + i).wait_send()
        for i in range(SENDS):
            keep_new(Q - SENDS + i).wait()
            new_partner(Q - SENDS + i, c).wait_send()
        for zz in range(4):

            @pl.when(z == zz)
            def _():
                for q in range(Q - SENDS, Q):
                    if zz < 3:
                        sum_right(q, zz).wait_send()
                        own_right(q, zz).wait_send()
                    if zz > 0:
                        sum_left(q, zz).wait_send()
                        own_left(q, zz).wait_send()
                    if zz in (1, 2):
                        on_right(q, zz).wait_send()
                        on_left(q, zz).wait_send()

    def slots(first, last, compute):
        @pl.loop(first, last)
        def _(t):
            compute(t)
            ready, p = chunk_after(t)

            @pl.when(ready)
            def _():
                @pl.when(p >= 2)
                def _():
                    to_partner(p - 2).wait_send()

                to_partner(p).start()

            sums(t)
            optimizer(t)
            spread(t)

    pl.run_scoped(forward, pltpu.VMEM((T, D), F32))
    @pl.when((z == 0) | (z == 3))
    def _():
        pl.semaphore_wait(bar, 2)

    @pl.when((z > 0) & (z < 3))
    def _():
        pl.semaphore_wait(bar, 3)

    slots(0, 36, first_layer)
    pl.run_scoped(
        lambda *bufs: slots(36, 54, lambda t: between(t, *bufs)),
        pltpu.VMEM((D, FF), BF16), pltpu.VMEM((D, FF), BF16),
        pltpu.VMEM((256, FF), BF16), pltpu.VMEM((256, FF), BF16), pltpu.VMEM((256, D), BF16),
    )
    slots(54, LAST, last_layer)
    last_waits()


def train(*operands):
    vm = pltpu.VMEM
    dma = pltpu.SemaphoreType.DMA
    any_ = pl.BlockSpec(memory_space=pl.ANY)
    shape = jax.ShapeDtypeStruct
    out_shape = [
        shape((CHUNKS, 2, 2, 4, ROWS, 128), BF16), *[shape(t.shape, F32) for t in operands[3:9]],
        shape((72, 32, T), BF16), shape((72, 32, T), BF16),
        shape((STEPS, T, CF), F32), shape((STEPS, T, CF), F32), shape((T, FF), BF16), shape((T, FF), BF16),
    ]
    return pl.pallas_call(
        train_kernel,
        in_specs=[any_] * len(operands),
        out_specs=[any_] * len(out_shape),
        out_shape=out_shape,
        scratch_shapes=[
            vm((T, D), BF16), vm((T, D), BF16), vm((T, D), BF16), vm((D, T), BF16),
            vm((T, CF), F32), vm((T, CF), F32), vm((T, CF), BF16), vm((T, CF), BF16),
            vm((2, D, CF), BF16), vm((2, D, CF), BF16), vm((2, CF, D), BF16),
            vm((8, 32, T), BF16), vm((2, 8, 32, T), BF16),
            vm((HELD, 2, 2, 4, ROWS, 128), BF16), vm((HELD, 2, 4, ROWS, 128), BF16),
            vm((RING, 4, ROWS, 128), BF16), vm((RING, 4, ROWS, 128), BF16),
            vm((SENDS, 4, ROWS, 128), BF16), vm((SENDS, 4, ROWS, 128), BF16),
            vm((RING, 4, ROWS, 128), BF16), vm((ROWS, 128), F32),
            vm((2, 112, 128), F32), vm((2, 112, 128), F32), vm((2, 112, 128), BF16),
            vm((2, 16, D), F32), vm((2, 16, D), F32), vm((2, 16, D), BF16),
            dma((3,)), dma((2, 3)), dma((2,)), dma((NRB, 2)), dma, dma((2,)), dma((2,)), dma((5,)),
            dma((2,)), dma((HELD,)), dma((SENDS,)), dma((RING,)), dma((SENDS,)), dma((RING,)),
            dma((SENDS,)), dma((RING,)), dma((SENDS,)), dma((RING,)), dma((SENDS,)), dma((RING,)),
            dma((SENDS,)), dma((RING,)), dma((SENDS,)), dma((RING,)), dma((SENDS,)), dma((2, 2)), dma((2, 3)),
        ],
        compiler_params=pltpu.CompilerParams(
            collective_id=0, has_side_effects=True, vmem_limit_bytes=VMEM_LIMIT
        ),
        name="train",
    )(*operands)


AHEAD = 12


def finish_kernel(
    wt, mg, mu, md, vg, vu, vd, owg, owu, owd, omg, omu, omd, ovg, ovu, ovd,
    wv, mgv, muv, mdv, vgv, vuv, vdv, columns, rows, w_sem, in_sem, out_sem, col_sem, row_sem,
):
    moments = ((mg, mgv, omg), (mu, muv, omu), (md, mdv, omd), (vg, vgv, ovg), (vu, vuv, ovu), (vd, vdv, ovd))
    pieces = [(i, layer) for layer in (1, 0) for i in range(6)]

    def take(i, layer):
        return pltpu.make_async_copy(moments[i][0].at[layer], moments[i][1].at[layer], in_sem.at[i, layer])

    def give(i, layer):
        return pltpu.make_async_copy(moments[i][1].at[layer], moments[i][2].at[layer], out_sem.at[i, layer])

    def chunk(p):
        return pltpu.make_async_copy(wt.at[p], wv.at[p], w_sem.at[p])

    def columns_out(out, layer, j, b):
        return pltpu.make_async_copy(columns.at[b], out.at[layer, :, pl.ds(pl.multiple_of(j * CF, CF), CF)], col_sem.at[b])

    def rows_out(layer, k, b):
        return pltpu.make_async_copy(rows.at[b], owd.at[layer, :, pl.ds(pl.multiple_of(k * 32, 32), 32), :], row_sem.at[b])

    for p in range(AHEAD):
        chunk(p).start()
    for i in range(2):
        take(*pieces[i]).start()

    def chunk_in(p):
        @pl.when(p + AHEAD < CHUNKS)
        def _():
            chunk(p + AHEAD).start()

        chunk(p).wait()

    for part in range(18):
        layer, base, n0 = 1 - part // 9, part // 9 * PER_LAYER, part % 9 * 3

        @pl.loop(0, 3)
        def _(i):
            n = n0 + i
            p = base + n
            chunk_in(p)
            if n0 < 18:
                b = n % 4

                @pl.when((n >= 4) | (base > 0))
                def _():
                    columns_out(owg, layer, 0, b).wait()

                for o in range(8):
                    for h in range(2):
                        columns[b, o * 112 : (o + 1) * 112, h * 128 : (h + 1) * 128] = wv[p, o % 2, h, o // 2]

                @pl.when(n % 2 == 0)
                def _():
                    columns_out(owg, layer, n // 2, b).start()

                @pl.when(n % 2 == 1)
                def _():
                    columns_out(owu, layer, n // 2, b).start()
            else:
                k = n - 18
                b = k % 4

                @pl.when((k >= 4) | (base > 0))
                def _():
                    rows_out(layer, 0, b).wait()

                for o in range(8):
                    for h in range(2):
                        for c in range(7):
                            rows[b, o, h * 16 : (h + 1) * 16, c * 128 : (c + 1) * 128] = wv[
                                p, o % 2, h, o // 2, c * 16 : (c + 1) * 16, :
                            ]
                rows_out(layer, k, b).start()

        if part < 12:
            take(*pieces[part]).wait()
            give(*pieces[part]).start()
            if part + 2 < 12:
                take(*pieces[part + 2]).start()

    for b in range(4):
        columns_out(owg, 0, 0, b).wait()
        rows_out(0, 0, b).wait()
    for piece in pieces:
        give(*piece).wait()


def finish(wtmp, *moments):
    vm, dma = pltpu.VMEM, pltpu.SemaphoreType.DMA
    any_ = pl.BlockSpec(memory_space=pl.ANY)
    out = pl.pallas_call(
        finish_kernel,
        in_specs=[any_] * 7,
        out_specs=[any_] * 9,
        out_shape=[
            jax.ShapeDtypeStruct((2, D, FF), BF16), jax.ShapeDtypeStruct((2, D, FF), BF16),
            jax.ShapeDtypeStruct((2, 8, 288, D), BF16),
            *[jax.ShapeDtypeStruct(t.shape, F32) for t in moments],
        ],
        scratch_shapes=[
            vm(wtmp.shape, BF16), *[vm(t.shape, F32) for t in moments], vm((4, D, CF), BF16), vm((4, 8, 32, D), BF16),
            dma((CHUNKS,)), dma((6, 2)), dma((6, 2)), dma((4,)), dma((4,)),
        ],
        compiler_params=pltpu.CompilerParams(vmem_limit_bytes=VMEM_LIMIT),
        name="finish",
    )(wtmp, *moments)
    return (out[0], out[1], out[2].reshape(2, FF, D), *out[3:])


def solution(mesh):
    def step(x, dy, wg, wu, wd, *moments):
        out = train(wg, wu, wd, *moments, x[0], dy[0])
        return finish(*out[:7])

    seq, whole, rows = P(("rep", "dp")), P(), P(None, "dp")
    return jax.shard_map(
        step, mesh=mesh,
        in_specs=(seq, seq, *[whole] * 3, *[rows] * 6),
        out_specs=(*[P("rep")] * 3, *[P("rep", "dp")] * 6),
        check_vma=False,
    )
```

```python
import jax
import jax.numpy as jnp
from jax import lax
from jax.experimental import pallas as pl
from jax.experimental.pallas import tpu as pltpu
from jax.sharding import PartitionSpec as P

MESH = pl.DeviceIdType.MESH
F32, BF16 = jnp.float32, jnp.bfloat16
T, D, FF = 2048, 896, 2304
CF = 256
STEPS = FF // CF
RB = 1024
NRB = T // RB
LANES = 128
HALF = 16
OWN = 32
ROWS = 112
PER_LAYER = 27
CHUNKS = 2 * PER_LAYER
Q = 2 * CHUNKS
LAG = 2
HELD = 8
RING = 2 * HELD
SENDS = 4
SPREAD = 4 + 6 * LAG
LAST = Q + SPREAD + 3
VMEM_LIMIT = 67043328


def nt(a, b):
    return lax.dot_general(a, b, (((1,), (1,)), ((), ())), preferred_element_type=F32)


def nn(a, b):
    return jnp.dot(a, b, preferred_element_type=F32)


def norm_scale(wide):
    return lax.rsqrt(jnp.mean(wide * wide, -1, keepdims=True) + 1e-6)


def sigmoid(g):
    return 1.0 / (1.0 + jnp.exp(-g))


def train_kernel(
    wg, wu, wd, mg, mu, md, vg, vu, vd, x, dy,
    wtmp, nmg, nmu, nmd, nvg, nvu, nvd, hid0_t, hid1_t, g0, u0, dg1, du1,
    xv, dyv, av, at, gbuf, ubuf, dg, du, wgj, wuj, wdj, hid_b, hid_c,
    grad, pin, rin, lin, rout, lout, news, gfin, mb, vb, wb, mbd, vbd, wbd,
    load_sem, w_sem, gu_sem, keep_sem, hw_sem, hc_sem, d_sem, da_sem,
    p_send, p_recv, r_send, r_recv, l_send, l_recv,
    or_send, or_recv, ol_send, ol_recv, ar_send, ar_recv, al_send, al_recv, ap_send, ap_recv, wo_sem, mo_sem, ad_sem,
):
    rep, me = lax.axis_index("rep"), lax.axis_index("dp")
    z, c = me // 2, me % 2
    partner = (rep, z * 2 + (1 - c))
    right = (rep, jnp.minimum(z + 1, 3) * 2 + c)
    left = (rep, jnp.maximum(z - 1, 0) * 2 + c)

    bar = pltpu.get_barrier_semaphore()
    pl.semaphore_signal(bar, inc=1, device_id=partner, device_id_type=MESH)

    @pl.when(z < 3)
    def _():
        pl.semaphore_signal(bar, inc=1, device_id=right, device_id_type=MESH)

    @pl.when(z > 0)
    def _():
        pl.semaphore_signal(bar, inc=1, device_id=left, device_id_type=MESH)

    valid = lambda q: (q >= 0) & (q < Q)

    def remote(src, dst, send, recv, to):
        return pltpu.make_async_remote_copy(
            src_ref=src, dst_ref=dst, send_sem=send, recv_sem=recv, device_id=to, device_id_type=MESH
        )

    def to_partner(p):
        e = p % HELD
        return remote(grad.at[e, 1 - c], pin.at[e], p_send.at[p % 2], p_recv.at[e], partner)

    def sum_right(q, frm):
        part = pl.ds(frm + 1, 3 - frm)
        return remote(rout.at[q % SENDS, part], rin.at[q % RING, part], r_send.at[q % SENDS], r_recv.at[q % RING], right)

    def sum_left(q, frm):
        part = pl.ds(0, frm)
        return remote(lout.at[q % SENDS, part], lin.at[q % RING, part], l_send.at[q % SENDS], l_recv.at[q % RING], left)

    def own_right(q, frm):
        here = news.at[q % RING, pl.ds(frm, 1)]
        return remote(here, here, or_send.at[q % SENDS], or_recv.at[q % RING], right)

    def own_left(q, frm):
        here = news.at[q % RING, pl.ds(frm, 1)]
        return remote(here, here, ol_send.at[q % SENDS], ol_recv.at[q % RING], left)

    def on_right(q, frm):
        here = news.at[q % RING, pl.ds(0, frm)]
        return remote(here, here, ar_send.at[q % SENDS], ar_recv.at[q % RING], right)

    def on_left(q, frm):
        here = news.at[q % RING, pl.ds(frm + 1, 3 - frm)]
        return remote(here, here, al_send.at[q % SENDS], al_recv.at[q % RING], left)

    def new_partner(q, core):
        return remote(
            news.at[q % RING], wtmp.at[q // 2, core, q % 2], ap_send.at[q % SENDS], ap_recv.at[q % RING], partner
        )

    def keep_new(q):
        return pltpu.make_async_copy(news.at[q % RING], wtmp.at[q // 2, c, q % 2], wo_sem.at[q % SENDS])

    def moments(q, act, new=False):
        p = q // 2
        layer = jnp.where(p < PER_LAYER, 1, 0)
        n = p % PER_LAYER
        s = q % 2
        cols = pl.ds(pl.multiple_of((n // 2) * CF + s * LANES, LANES), LANES)
        for which, (m, v, w, nm, nv) in enumerate(((mg, vg, wg, nmg, nvg), (mu, vu, wu, nmu, nvu))):

            @pl.when((n < 18) & (n % 2 == which))
            def _():
                if new:
                    act(pltpu.make_async_copy(mb.at[s], nm.at[layer, :, cols], mo_sem.at[s, 0]))
                    act(pltpu.make_async_copy(vb.at[s], nv.at[layer, :, cols], mo_sem.at[s, 1]))
                else:
                    own = pl.ds(pl.multiple_of(me * ROWS, HALF), ROWS)
                    act(pltpu.make_async_copy(m.at[layer, :, cols], mb.at[s], ad_sem.at[s, 0]))
                    act(pltpu.make_async_copy(v.at[layer, :, cols], vb.at[s], ad_sem.at[s, 1]))
                    act(pltpu.make_async_copy(w.at[layer, own, cols], wb.at[s], ad_sem.at[s, 2]))

        @pl.when(n >= 18)
        def _():
            rows = pl.ds(pl.multiple_of((n - 18) * OWN + s * HALF, HALF), HALF)
            if new:
                act(pltpu.make_async_copy(mbd.at[s], nmd.at[layer, rows, :], mo_sem.at[s, 0]))
                act(pltpu.make_async_copy(vbd.at[s], nvd.at[layer, rows, :], mo_sem.at[s, 1]))
            else:
                own = pl.ds(pl.multiple_of(me * 288 + (n - 18) * OWN + s * HALF, HALF), HALF)
                act(pltpu.make_async_copy(md.at[layer, rows, :], mbd.at[s], ad_sem.at[s, 0]))
                act(pltpu.make_async_copy(vd.at[layer, rows, :], vbd.at[s], ad_sem.at[s, 1]))
                act(pltpu.make_async_copy(wd.at[layer, own, :], wbd.at[s], ad_sem.at[s, 2]))

    def adamw(w, m, v, g):
        m = 0.9 * m + 0.1 * g
        v = 0.95 * v + 0.05 * g * g
        step = m * lax.rsqrt(v + 1e-8) + 0.1 * w
        return (w - 0.02 * step).astype(BF16), m, v

    def weights_of(n, act):
        s = n % 2
        cols = pl.ds(pl.multiple_of((n % STEPS) * CF, CF), CF)
        layer = jnp.where((n >= STEPS) & (n < 2 * STEPS), 1, 0)

        @pl.when(n < 2 * STEPS)
        def _():
            act(pltpu.make_async_copy(wg.at[layer, :, cols], wgj.at[s], w_sem.at[s, 0]))
            act(pltpu.make_async_copy(wu.at[layer, :, cols], wuj.at[s], w_sem.at[s, 1]))

        @pl.when(n < 3 * STEPS)
        def _():
            act(pltpu.make_async_copy(wd.at[layer, cols, :], wdj.at[s], w_sem.at[s, 2]))

    def saved_of(j, act):
        @pl.when(j < STEPS)
        def _():
            act(pltpu.make_async_copy(g0.at[j], gbuf, gu_sem.at[0]))
            act(pltpu.make_async_copy(u0.at[j], ubuf, gu_sem.at[1]))

    def keep_saved(j, r):
        rows = pl.ds(pl.multiple_of(r * RB, RB), RB)
        return (
            pltpu.make_async_copy(gbuf.at[rows], g0.at[j, rows], keep_sem.at[r, 0]),
            pltpu.make_async_copy(ubuf.at[rows], u0.at[j, rows], keep_sem.at[r, 1]),
        )

    def keep_hidden0(j):
        return pltpu.make_async_copy(hid_c.at[j % 2], hid0_t.at[pl.ds(j * 8, 8)], hc_sem.at[j % 2])

    def keep_hidden(j):
        return pltpu.make_async_copy(hid_b, hid1_t.at[pl.ds(j * 8, 8)], hw_sem)

    def keep_d(j):
        cols = pl.ds(pl.multiple_of(j * CF, CF), CF)
        return (
            pltpu.make_async_copy(dg, dg1.at[:, cols], d_sem.at[0]),
            pltpu.make_async_copy(du, du1.at[:, cols], d_sem.at[1]),
        )

    def hidden_of(src, k, start):
        s = k % 2
        if start:
            for o in range(8):
                pltpu.make_async_copy(src.at[o * 9 + k], hid_c.at[s, o], hc_sem.at[s]).start()
        else:
            pltpu.make_async_copy(src.at[pl.ds(0, 8)], hid_c.at[s], hc_sem.at[s]).wait()

    load_dy = pltpu.make_async_copy(dy, dyv, load_sem.at[2])

    start = lambda copy: copy.start()
    wait = lambda copy: copy.wait()

    def grad_columns(p, d):
        out = nn(at[:], d[:]).astype(BF16)
        for o in range(8):
            for h in range(2):
                grad[p % HELD, o % 2, h, o // 2] = out[o * ROWS : (o + 1) * ROWS, h * LANES : (h + 1) * LANES]

    def grad_rows(p, k, d):
        out = nn(hid_c[k % 2].reshape(CF, T), d[:]).astype(BF16)
        for o in range(8):
            for h in range(2):
                for i in range(7):
                    grad[p % HELD, o % 2, h, o // 2, i * HALF : (i + 1) * HALF, :] = out[
                        o * OWN + h * HALF : o * OWN + h * HALF + HALF, i * LANES : (i + 1) * LANES
                    ]

    def hidden_back(g, u, dp):
        s = sigmoid(g)
        act = g * s
        return act, (dp * u * (s + act * (1.0 - s))).astype(BF16), (dp * act).astype(BF16)

    def rows_of(r, n=RB):
        return pl.ds(pl.multiple_of(r * n, n), n)

    def forward(acc):
        weights_of(0, start)
        halves = [pltpu.make_async_copy(x.at[rows_of(r)], xv.at[rows_of(r)], load_sem.at[r]) for r in range(NRB)]
        for copy in halves:
            copy.start()
        load_dy.start()
        def normed_input(r):
            wide = xv[rows_of(r), :].astype(F32)
            av[rows_of(r), :] = (wide * norm_scale(wide)).astype(BF16)

        def output(r):
            rows = rows_of(r)
            y = acc[rows, :].astype(BF16).astype(F32)
            h = (xv[rows, :].astype(F32) + y).astype(BF16)
            xv[rows, :] = h
            wide = h.astype(F32)
            av[rows, :] = (wide * norm_scale(wide)).astype(BF16)

        def step(i, first, beside=None):
            j, r = i // NRB, i % NRB
            b = j % 2
            rows = rows_of(r)

            @pl.when(r == 0)
            def _():
                weights_of(j + 1, start)
                weights_of(j, wait)

                @pl.when(j > 1)
                def _():
                    keep_hidden0(j - 2).wait()

            @pl.when(j > 0)
            def _():
                for copy in keep_saved(j - 1, r):
                    copy.wait()

            a = av[rows, :]
            g = nn(a, wgj[b])
            u = nn(a, wuj[b])
            gbuf[rows, :] = g
            ubuf[rows, :] = u
            hid = (g * sigmoid(g) * u).astype(BF16)
            hid_c[b, :, :, rows] = hid.T.reshape(8, OWN, RB)
            y = nn(hid, wdj[b])
            acc[rows, :] = y if first else acc[rows, :] + y
            if beside:
                beside()
            for copy in keep_saved(j, r):
                copy.start()

            @pl.when(r == NRB - 1)
            def _():
                keep_hidden0(j).start()

        halves[0].wait()
        normed_input(0)
        halves[1].wait()
        step(0, True, lambda: normed_input(1))
        step(1, True)

        @pl.loop(NRB, NRB * STEPS - 1)
        def _(i):
            step(i, False)

        step(NRB * STEPS - 1, False, lambda: output(0))
        output(1)
        load_dy.wait()

    def first_layer(t):
        j = t // 4
        b = (j + 1) % 2

        @pl.when(t % 4 == 0)
        def _():
            weights_of(STEPS + j + 1, start)
            weights_of(STEPS + j, wait)

            @pl.when(j > 0)
            def _():
                keep_hidden(j - 1).wait()
                for copy in keep_d(j - 1):
                    copy.wait()

        @pl.when(t % 4 < 2)
        def _():
            rows = rows_of(t % 4)
            a = av[rows, :]
            at[:, rows] = a.T
            g = nn(a, wgj[b])
            u = nn(a, wuj[b])
            dp = nt(dyv[rows, :], wdj[b]).astype(BF16).astype(F32)
            act, dgr, dur = hidden_back(g, u, dp)
            hid_b[:, :, rows] = (act * u).astype(BF16).T.reshape(8, OWN, RB)
            dg[rows, :] = dgr
            du[rows, :] = dur

        @pl.when(t % 4 == 2)
        def _():
            keep_hidden(j).start()
            for copy in keep_d(j):
                copy.start()
            grad_columns(2 * j, dg)

        @pl.when(t % 4 == 3)
        def _():
            grad_columns(2 * j + 1, du)

            @pl.when(j == STEPS - 1)
            def _():
                keep_hidden(STEPS - 1).wait()
                for copy in keep_d(STEPS - 1):
                    copy.wait()
                for r in range(NRB):
                    for copy in keep_saved(STEPS - 1, r):
                        copy.wait()
                for i in range(2):
                    keep_hidden0(STEPS - 2 + i).wait()
                hidden_of(hid1_t, 0, True)
                saved_of(0, start)

    def between(t, wgl, wul, dgb, dub, xb):
        k = (t - 36) // 2
        block = lambda i: (
            pltpu.make_async_copy(dg1.at[rows_of(i, CF)], dgb, da_sem.at[2]),
            pltpu.make_async_copy(du1.at[rows_of(i, CF)], dub, da_sem.at[3]),
            pltpu.make_async_copy(x.at[rows_of(i, CF)], xb, da_sem.at[4]),
        )
        weights = (
            pltpu.make_async_copy(wg.at[1], wgl, da_sem.at[0]),
            pltpu.make_async_copy(wu.at[1], wul, da_sem.at[1]),
        )

        @pl.when(t == 36)
        def _():
            for copy in (*weights, *block(0)):
                copy.start()

        @pl.when(t == 38)
        def _():
            for copy in weights:
                copy.wait()

        @pl.when((k > 0) & (t % 2 == 0))
        def _():
            for copy in block(k - 1):
                copy.wait()
            by_g = nt(wgl[:], dgb[:])
            by_u = nt(wul[:], dub[:])
            da = by_g.astype(BF16).astype(F32) + by_u.astype(BF16).astype(F32)
            da = da.astype(BF16).T.astype(F32)
            rows = rows_of(k - 1, CF)
            wide = xv[rows, :].astype(F32)
            scale = norm_scale(wide)
            along = jnp.sum(da * wide, -1, keepdims=True) * (scale * scale * scale) * (-1.0 / D)
            back = (da * scale + wide * along).astype(BF16)
            xv[rows, :] = (dyv[rows, :].astype(F32) + back.astype(F32)).astype(BF16)
            wide = xb[:].astype(F32)
            at[:, rows] = (wide * norm_scale(wide)).astype(BF16).T

            @pl.when(k < 8)
            def _():
                for copy in block(k):
                    copy.start()

        @pl.when(t % 2 == 1)
        def _():
            @pl.when(k < 8)
            def _():
                hidden_of(hid1_t, k + 1, True)

            hidden_of(hid1_t, k, False)
            grad_rows(18 + k, k, dyv)

    def last_layer(t):
        j = (t - 54) // 4
        b = j % 2
        turn = (t - 54) % 4
        k = (t - 90) // 2

        @pl.when((t < 90) & (turn == 0))
        def _():
            weights_of(2 * STEPS + j + 1, start)
            weights_of(2 * STEPS + j, wait)
            saved_of(j, wait)

        @pl.when((t < 90) & (turn < 2))
        def _():
            rows = rows_of(turn)
            dp = nt(xv[rows, :], wdj[b]).astype(BF16).astype(F32)
            _, dgr, dur = hidden_back(gbuf[rows, :], ubuf[rows, :], dp)
            dg[rows, :] = dgr
            du[rows, :] = dur

        @pl.when((t < 90) & (turn == 2))
        def _():
            saved_of(j + 1, start)
            grad_columns(PER_LAYER + 2 * j, dg)

        @pl.when((t < 90) & (turn == 3))
        def _():
            grad_columns(PER_LAYER + 2 * j + 1, du)

            @pl.when(t == 89)
            def _():
                hidden_of(hid0_t, 0, True)

        @pl.when((t >= 90) & (t < Q) & (t % 2 == 1))
        def _():
            @pl.when(k < 8)
            def _():
                hidden_of(hid0_t, k + 1, True)

            hidden_of(hid0_t, k, False)
            grad_rows(PER_LAYER + 18 + k, k, xv)

    def chunk_after(t):
        n = t % 54
        pair = n < 36
        return (t < Q) & jnp.where(pair, n % 4 >= 2, n % 2 == 1), (t // 54) * PER_LAYER + jnp.where(
            pair, 2 * (n // 4) + n % 2, n // 2
        )

    f32 = lambda t: t.astype(F32)

    def sums(t):
        q = t - 3

        @pl.when(valid(q) & (q % 2 == 0))
        def _():
            to_partner(q // 2).wait_recv()

        qr = t - 3 - LAG * z
        ql = t - 3 - LAG * (3 - z)

        def own(q, to):
            e = (q // 2) % HELD
            return f32(grad[e, c, q % 2, to]) + f32(pin[e, q % 2, to])

        for zz in range(4):

            @pl.when(z == zz)
            def _():
                @pl.when(valid(qr))
                def _():
                    if zz > 0:
                        sum_right(qr, zz - 1).wait_recv()
                    if zz < 3:

                        @pl.when(qr >= SENDS)
                        def _():
                            sum_right(qr - SENDS, zz).wait_send()

                        for to in range(zz + 1, 4):
                            total = own(qr, to)
                            if zz > 0:
                                total = total + f32(rin[qr % RING, to])
                            rout[qr % SENDS, to] = total.astype(BF16)
                        sum_right(qr, zz).start()

                @pl.when(valid(ql))
                def _():
                    if zz < 3:
                        sum_left(ql, zz + 1).wait_recv()
                    if zz > 0:

                        @pl.when(ql >= SENDS)
                        def _():
                            sum_left(ql - SENDS, zz).wait_send()

                        for to in range(zz):
                            total = own(ql, to)
                            if zz < 3:
                                total = total + f32(lin[ql % RING, to])
                            lout[ql % SENDS, to] = total.astype(BF16)
                        sum_left(ql, zz).start()

    def optimizer(t):
        q = t - 3 - LAG * jnp.maximum(z, 3 - z)

        @pl.when((q >= 1) & (q <= Q))
        def _():
            moments(q - 1, wait, new=True)

        @pl.when(valid(q + 1))
        def _():
            moments(q + 1, start)

        @pl.when(valid(q))
        def _():
            e, h = (q // 2) % HELD, q % 2
            gfin[:] = f32(grad[e, c, h, z]) + f32(pin[e, h, z])

            @pl.when(z > 0)
            def _():
                gfin[:] += f32(rin[q % RING, z])

            @pl.when(z < 3)
            def _():
                gfin[:] += f32(lin[q % RING, z])

            moments(q, wait)
            n = (q // 2) % PER_LAYER

            @pl.when(n < 18)
            def _():
                g = f32(gfin[:].astype(BF16))
                news[q % RING, z], mb[h], vb[h] = adamw(f32(wb[h]), mb[h], vb[h], g)

            @pl.when(n >= 18)
            def _():
                for i in range(7):
                    lanes = slice(i * LANES, (i + 1) * LANES)
                    part = slice(i * HALF, (i + 1) * HALF)
                    g = f32(gfin[part, :].astype(BF16))
                    news[q % RING, z, part, :], mbd[h, :, lanes], vbd[h, :, lanes] = adamw(
                        f32(wbd[h, :, lanes]), mbd[h, :, lanes], vbd[h, :, lanes], g
                    )

            moments(q, start, new=True)

    def send(copy, q, frm):
        @pl.when(q >= SENDS)
        def _():
            copy(q - SENDS, frm).wait_send()

        copy(q, frm).start()

    def spread(t):
        for zz in range(4):

            @pl.when(z == zz)
            def _():
                q = t - 4 - LAG * max(zz, 3 - zz)

                @pl.when(valid(q))
                def _():
                    if zz < 3:
                        send(own_right, q, zz)
                    if zz > 0:
                        send(own_left, q, zz)

                if zz in (1, 2):
                    near, far = t - 4 - 4 * LAG, t - 4 - 5 * LAG
                    qr, ql = (near, far) if zz == 1 else (far, near)

                    @pl.when(valid(qr))
                    def _():
                        own_right(qr, zz - 1).wait_recv()
                        if zz == 2:
                            on_right(qr, 1).wait_recv()
                        send(on_right, qr, zz)

                    @pl.when(valid(ql))
                    def _():
                        own_left(ql, zz + 1).wait_recv()
                        if zz == 1:
                            on_left(ql, 2).wait_recv()
                        send(on_left, ql, zz)
                else:
                    q = t - SPREAD

                    @pl.when(valid(q))
                    def _():
                        if zz == 3:
                            own_right(q, 2).wait_recv()
                            on_right(q, 2).wait_recv()
                        else:
                            own_left(q, 1).wait_recv()
                            on_left(q, 1).wait_recv()

        q = t - SPREAD

        @pl.when(valid(q))
        def _():
            @pl.when(q >= SENDS)
            def _():
                new_partner(q - SENDS, c).wait_send()
                keep_new(q - SENDS).wait()

            new_partner(q, c).start()
            keep_new(q).start()

        @pl.when(valid(q - 2))
        def _():
            new_partner(q - 2, 1 - c).wait_recv()

    def last_waits():
        for i in range(2):
            to_partner(CHUNKS - 2 + i).wait_send()
        for i in range(SENDS):
            keep_new(Q - SENDS + i).wait()
            new_partner(Q - SENDS + i, c).wait_send()
        for zz in range(4):

            @pl.when(z == zz)
            def _():
                for q in range(Q - SENDS, Q):
                    if zz < 3:
                        sum_right(q, zz).wait_send()
                        own_right(q, zz).wait_send()
                    if zz > 0:
                        sum_left(q, zz).wait_send()
                        own_left(q, zz).wait_send()
                    if zz in (1, 2):
                        on_right(q, zz).wait_send()
                        on_left(q, zz).wait_send()

    def slots(first, last, compute):
        @pl.loop(first, last)
        def _(t):
            compute(t)
            ready, p = chunk_after(t)

            @pl.when(ready)
            def _():
                @pl.when(p >= 2)
                def _():
                    to_partner(p - 2).wait_send()

                to_partner(p).start()

            sums(t)
            optimizer(t)
            spread(t)

    pl.run_scoped(forward, pltpu.VMEM((T, D), F32))
    @pl.when((z == 0) | (z == 3))
    def _():
        pl.semaphore_wait(bar, 2)

    @pl.when((z > 0) & (z < 3))
    def _():
        pl.semaphore_wait(bar, 3)

    slots(0, 36, first_layer)
    pl.run_scoped(
        lambda *bufs: slots(36, 54, lambda t: between(t, *bufs)),
        pltpu.VMEM((D, FF), BF16), pltpu.VMEM((D, FF), BF16),
        pltpu.VMEM((CF, FF), BF16), pltpu.VMEM((CF, FF), BF16), pltpu.VMEM((CF, D), BF16),
    )
    slots(54, LAST, last_layer)
    last_waits()


def train(*operands):
    vm = pltpu.VMEM
    dma = pltpu.SemaphoreType.DMA
    any_ = pl.BlockSpec(memory_space=pl.ANY)
    shape = jax.ShapeDtypeStruct
    out_shape = [
        shape((CHUNKS, 2, 2, 4, ROWS, LANES), BF16), *[shape(t.shape, F32) for t in operands[3:9]],
        shape((72, OWN, T), BF16), shape((72, OWN, T), BF16),
        shape((STEPS, T, CF), F32), shape((STEPS, T, CF), F32), shape((T, FF), BF16), shape((T, FF), BF16),
    ]
    return pl.pallas_call(
        train_kernel,
        in_specs=[any_] * len(operands),
        out_specs=[any_] * len(out_shape),
        out_shape=out_shape,
        scratch_shapes=[
            vm((T, D), BF16), vm((T, D), BF16), vm((T, D), BF16), vm((D, T), BF16),
            vm((T, CF), F32), vm((T, CF), F32), vm((T, CF), BF16), vm((T, CF), BF16),
            vm((2, D, CF), BF16), vm((2, D, CF), BF16), vm((2, CF, D), BF16),
            vm((8, OWN, T), BF16), vm((2, 8, OWN, T), BF16),
            vm((HELD, 2, 2, 4, ROWS, LANES), BF16), vm((HELD, 2, 4, ROWS, LANES), BF16),
            vm((RING, 4, ROWS, LANES), BF16), vm((RING, 4, ROWS, LANES), BF16),
            vm((SENDS, 4, ROWS, LANES), BF16), vm((SENDS, 4, ROWS, LANES), BF16),
            vm((RING, 4, ROWS, LANES), BF16), vm((ROWS, LANES), F32),
            vm((2, ROWS, LANES), F32), vm((2, ROWS, LANES), F32), vm((2, ROWS, LANES), BF16),
            vm((2, HALF, D), F32), vm((2, HALF, D), F32), vm((2, HALF, D), BF16),
            dma((3,)), dma((2, 3)), dma((2,)), dma((NRB, 2)), dma, dma((2,)), dma((2,)), dma((5,)),
            dma((2,)), dma((HELD,)), dma((SENDS,)), dma((RING,)), dma((SENDS,)), dma((RING,)),
            dma((SENDS,)), dma((RING,)), dma((SENDS,)), dma((RING,)), dma((SENDS,)), dma((RING,)),
            dma((SENDS,)), dma((RING,)), dma((SENDS,)), dma((RING,)), dma((SENDS,)), dma((2, 2)), dma((2, 3)),
        ],
        compiler_params=pltpu.CompilerParams(
            collective_id=0, has_side_effects=True, vmem_limit_bytes=VMEM_LIMIT
        ),
        name="train",
    )(*operands)


AHEAD = 12


def finish_kernel(
    wt, mg, mu, md, vg, vu, vd, owg, owu, owd, omg, omu, omd, ovg, ovu, ovd,
    wv, mgv, muv, mdv, vgv, vuv, vdv, columns, rows, w_sem, in_sem, out_sem, col_sem, row_sem,
):
    moments = ((mg, mgv, omg), (mu, muv, omu), (md, mdv, omd), (vg, vgv, ovg), (vu, vuv, ovu), (vd, vdv, ovd))
    pieces = [(i, layer) for layer in (1, 0) for i in range(6)]

    def take(i, layer):
        return pltpu.make_async_copy(moments[i][0].at[layer], moments[i][1].at[layer], in_sem.at[i, layer])

    def give(i, layer):
        return pltpu.make_async_copy(moments[i][1].at[layer], moments[i][2].at[layer], out_sem.at[i, layer])

    def chunk(p):
        return pltpu.make_async_copy(wt.at[p], wv.at[p], w_sem.at[p])

    def columns_out(out, layer, j, b):
        return pltpu.make_async_copy(columns.at[b], out.at[layer, :, pl.ds(pl.multiple_of(j * CF, CF), CF)], col_sem.at[b])

    def rows_out(layer, k, b):
        return pltpu.make_async_copy(rows.at[b], owd.at[layer, :, pl.ds(pl.multiple_of(k * OWN, OWN), OWN), :], row_sem.at[b])

    for p in range(AHEAD):
        chunk(p).start()
    for i in range(2):
        take(*pieces[i]).start()

    def chunk_in(p):
        @pl.when(p + AHEAD < CHUNKS)
        def _():
            chunk(p + AHEAD).start()

        chunk(p).wait()

    for part in range(18):
        layer, base, n0 = 1 - part // 9, part // 9 * PER_LAYER, part % 9 * 3

        @pl.loop(0, 3)
        def _(i):
            n = n0 + i
            p = base + n
            chunk_in(p)
            if n0 < 18:
                b = n % 4

                @pl.when((n >= 4) | (base > 0))
                def _():
                    columns_out(owg, layer, 0, b).wait()

                for o in range(8):
                    for h in range(2):
                        columns[b, o * ROWS : (o + 1) * ROWS, h * LANES : (h + 1) * LANES] = wv[p, o % 2, h, o // 2]

                @pl.when(n % 2 == 0)
                def _():
                    columns_out(owg, layer, n // 2, b).start()

                @pl.when(n % 2 == 1)
                def _():
                    columns_out(owu, layer, n // 2, b).start()
            else:
                k = n - 18
                b = k % 4

                @pl.when((k >= 4) | (base > 0))
                def _():
                    rows_out(layer, 0, b).wait()

                for o in range(8):
                    for h in range(2):
                        for c in range(7):
                            rows[b, o, h * HALF : (h + 1) * HALF, c * LANES : (c + 1) * LANES] = wv[
                                p, o % 2, h, o // 2, c * HALF : (c + 1) * HALF, :
                            ]
                rows_out(layer, k, b).start()

        if part < 12:
            take(*pieces[part]).wait()
            give(*pieces[part]).start()
            if part + 2 < 12:
                take(*pieces[part + 2]).start()

    for b in range(4):
        columns_out(owg, 0, 0, b).wait()
        rows_out(0, 0, b).wait()
    for piece in pieces:
        give(*piece).wait()


def finish(wtmp, *moments):
    vm, dma = pltpu.VMEM, pltpu.SemaphoreType.DMA
    any_ = pl.BlockSpec(memory_space=pl.ANY)
    out = pl.pallas_call(
        finish_kernel,
        in_specs=[any_] * 7,
        out_specs=[any_] * 9,
        out_shape=[
            jax.ShapeDtypeStruct((2, D, FF), BF16), jax.ShapeDtypeStruct((2, D, FF), BF16),
            jax.ShapeDtypeStruct((2, 8, 288, D), BF16),
            *[jax.ShapeDtypeStruct(t.shape, F32) for t in moments],
        ],
        scratch_shapes=[
            vm(wtmp.shape, BF16), *[vm(t.shape, F32) for t in moments], vm((4, D, CF), BF16), vm((4, 8, OWN, D), BF16),
            dma((CHUNKS,)), dma((6, 2)), dma((6, 2)), dma((4,)), dma((4,)),
        ],
        compiler_params=pltpu.CompilerParams(vmem_limit_bytes=VMEM_LIMIT),
        name="finish",
    )(wtmp, *moments)
    return (out[0], out[1], out[2].reshape(2, FF, D), *out[3:])


def solution(mesh):
    def step(x, dy, wg, wu, wd, *moments):
        out = train(wg, wu, wd, *moments, x[0], dy[0])
        return finish(*out[:7])

    seq, whole, rows = P(("rep", "dp")), P(), P(None, "dp")
    return jax.shard_map(
        step, mesh=mesh,
        in_specs=(seq, seq, *[whole] * 3, *[rows] * 6),
        out_specs=(*[P("rep")] * 3, *[P("rep", "dp")] * 6),
        check_vma=False,
    )
```

```python
import jax
import jax.numpy as jnp
from jax import lax
from jax.experimental import pallas as pl
from jax.experimental.pallas import tpu as pltpu
from jax.sharding import PartitionSpec as P

MESH = pl.DeviceIdType.MESH
F32, BF16 = jnp.float32, jnp.bfloat16
T, D, FF = 2048, 896, 2304
CF = 256
STEPS = FF // CF
RB = 1024
NRB = T // RB
LANES = 128
HALF = 16
OWN = 32
ROWS = 112
PER_LAYER = 27
CHUNKS = 2 * PER_LAYER
Q = 2 * CHUNKS
LAG = 2
HELD = 7
RING = 2 * HELD
SENDS = 4
OUT = 3
SPREAD = 4 + 6 * LAG
LAST = Q + SPREAD + 3
VMEM_LIMIT = 48000000


def nt(a, b):
    return lax.dot_general(a, b, (((1,), (1,)), ((), ())), preferred_element_type=F32)


def nn(a, b):
    return jnp.dot(a, b, preferred_element_type=F32)


def norm_scale(wide):
    return lax.rsqrt(jnp.mean(wide * wide, -1, keepdims=True) + 1e-6)


def sigmoid(g):
    return 1.0 / (1.0 + jnp.exp(-g))


def train_kernel(
    wg, wu, wd, mg, mu, md, vg, vu, vd, x, dy,
    wtmp, nmg, nmu, nmd, nvg, nvu, nvd, hid0_t, hid1_t, dg1, du1,
    xv, dyv, av, at, dg, du, wgj, wuj, wdj, hid_c,
    grad, pin, sums_in, rout, lout, news, gfin, mb, vb, wb, mbd, vbd, wbd,
    load_sem, w_sem, hw_sem, hc_sem, d_sem, da_sem,
    p_send, p_recv, r_send, r_recv, l_send, l_recv,
    or_send, or_recv, ol_send, ol_recv, ar_send, ar_recv, al_send, al_recv, ap_send, ap_recv, wo_sem, mo_sem, ad_sem,
):
    rep, me = lax.axis_index("rep"), lax.axis_index("dp")
    z, c = me // 2, me % 2
    partner = (rep, z * 2 + (1 - c))
    right = (rep, jnp.minimum(z + 1, 3) * 2 + c)
    left = (rep, jnp.maximum(z - 1, 0) * 2 + c)

    bar = pltpu.get_barrier_semaphore()
    pl.semaphore_signal(bar, inc=1, device_id=partner, device_id_type=MESH)

    @pl.when(z < 3)
    def _():
        pl.semaphore_signal(bar, inc=1, device_id=right, device_id_type=MESH)

    @pl.when(z > 0)
    def _():
        pl.semaphore_signal(bar, inc=1, device_id=left, device_id_type=MESH)

    valid = lambda q: (q >= 0) & (q < Q)

    def remote(src, dst, send, recv, to):
        return pltpu.make_async_remote_copy(
            src_ref=src, dst_ref=dst, send_sem=send, recv_sem=recv, device_id=to, device_id_type=MESH
        )

    def to_partner(p):
        e = p % HELD
        return remote(grad.at[e, 1 - c], pin.at[e], p_send.at[p % 2], p_recv.at[e], partner)

    def sum_right(q, frm):
        part = pl.ds(frm, 3 - frm)
        there = pl.ds(0, 3 - frm)
        return remote(rout.at[q % OUT, part], sums_in.at[q % RING, there], r_send.at[q % OUT], r_recv.at[q % RING], right)

    def sum_left(q, frm):
        part = pl.ds(0, frm)
        there = pl.ds(5 - frm, frm)
        return remote(lout.at[q % OUT, part], sums_in.at[q % RING, there], l_send.at[q % OUT], l_recv.at[q % RING], left)

    def own_right(q, frm):
        here = news.at[q % RING, pl.ds(frm, 1)]
        return remote(here, here, or_send.at[q % SENDS], or_recv.at[q % RING], right)

    def own_left(q, frm):
        here = news.at[q % RING, pl.ds(frm, 1)]
        return remote(here, here, ol_send.at[q % SENDS], ol_recv.at[q % RING], left)

    def on_right(q, frm):
        here = news.at[q % RING, pl.ds(0, frm)]
        return remote(here, here, ar_send.at[q % SENDS], ar_recv.at[q % RING], right)

    def on_left(q, frm):
        here = news.at[q % RING, pl.ds(frm + 1, 3 - frm)]
        return remote(here, here, al_send.at[q % SENDS], al_recv.at[q % RING], left)

    def new_partner(q, core):
        return remote(
            news.at[q % RING], wtmp.at[q // 2, core, q % 2], ap_send.at[q % 2], ap_recv.at[q % RING], partner
        )

    def keep_new(q):
        return pltpu.make_async_copy(news.at[q % RING], wtmp.at[q // 2, c, q % 2], wo_sem.at[q % 2])

    def place(q):
        p, s = q // 2, q % 2
        n = p % PER_LAYER
        cols = pl.ds(pl.multiple_of((n // 2) * CF + s * LANES, LANES), LANES)
        rows = pl.ds(pl.multiple_of(jnp.maximum(n - 18, 0) * OWN + s * HALF, HALF), HALF)
        return jnp.where(p < PER_LAYER, 1, 0), n, s, cols, rows

    def moments(q, act):
        layer, n, s, cols, rows = place(q)
        for which, (m, v, w) in enumerate(((mg, vg, wg), (mu, vu, wu))):

            @pl.when((n < 18) & (n % 2 == which))
            def _():
                own = pl.ds(pl.multiple_of(me * ROWS, HALF), ROWS)
                act(pltpu.make_async_copy(m.at[layer, :, cols], mb.at[s], ad_sem.at[s, 0]))
                act(pltpu.make_async_copy(v.at[layer, :, cols], vb.at[s], ad_sem.at[s, 1]))
                act(pltpu.make_async_copy(w.at[layer, own, cols], wb.at[s], ad_sem.at[s, 2]))

        @pl.when(n >= 18)
        def _():
            own = pl.ds(pl.multiple_of(me * 288 + (n - 18) * OWN + s * HALF, HALF), HALF)
            act(pltpu.make_async_copy(md.at[layer, rows, :], mbd.at[s], ad_sem.at[s, 0]))
            act(pltpu.make_async_copy(vd.at[layer, rows, :], vbd.at[s], ad_sem.at[s, 1]))
            act(pltpu.make_async_copy(wd.at[layer, own, :], wbd.at[s], ad_sem.at[s, 2]))

    def keep_moments(q, act):
        layer, n, s, cols, rows = place(q)

        @pl.when((n < 18) & (n % 2 == 1))
        def _():
            act(pltpu.make_async_copy(vb.at[s], nvu.at[layer, :, cols], mo_sem.at[s]))

        @pl.when(n >= 18)
        def _():
            act(pltpu.make_async_copy(vbd.at[s], nvd.at[layer, rows, :], mo_sem.at[s]))

    def adamw(w, m, v, g):
        m = 0.9 * m + 0.1 * g
        v = 0.95 * v + 0.05 * g * g
        step = m * lax.rsqrt(v + 1e-8) + 0.1 * w
        return (w - 0.02 * step).astype(BF16), m, v

    def weights_of(n, act):
        s = n % 2
        cols = pl.ds(pl.multiple_of((n % STEPS) * CF, CF), CF)
        layer = jnp.where((n >= STEPS) & (n < 2 * STEPS), 1, 0)

        @pl.when(n < 3 * STEPS)
        def _():
            act(pltpu.make_async_copy(wg.at[layer, :, cols], wgj.at[s], w_sem.at[s, 0]))
            act(pltpu.make_async_copy(wu.at[layer, :, cols], wuj.at[s], w_sem.at[s, 1]))
            act(pltpu.make_async_copy(wd.at[layer, cols, :], wdj.at[s], w_sem.at[s, 2]))

    def keep_hidden0(j):
        return pltpu.make_async_copy(hid_c.at[j % 2], hid0_t.at[pl.ds(j * 8, 8)], hc_sem.at[j % 2])

    def keep_hidden(j):
        return pltpu.make_async_copy(hid_c.at[1], hid1_t.at[pl.ds(j * 8, 8)], hw_sem)

    def keep_d(j):
        cols = pl.ds(pl.multiple_of(j * CF, CF), CF)
        return (
            pltpu.make_async_copy(dg, dg1.at[:, cols], d_sem.at[0]),
            pltpu.make_async_copy(du, du1.at[:, cols], d_sem.at[1]),
        )

    def hidden_of(src, k, start):
        s = k % 2
        if start:
            for o in range(8):
                pltpu.make_async_copy(src.at[o * 9 + k], hid_c.at[s, o], hc_sem.at[s]).start()
        else:
            pltpu.make_async_copy(src.at[pl.ds(0, 8)], hid_c.at[s], hc_sem.at[s]).wait()

    load_dy = pltpu.make_async_copy(dy, dyv, load_sem.at[2])

    start = lambda copy: copy.start()
    wait = lambda copy: copy.wait()

    def grad_columns(p, d):
        out = nn(at[:], d[:]).astype(BF16)
        for o in range(8):
            for h in range(2):
                grad[p % HELD, o % 2, h, o // 2] = out[o * ROWS : (o + 1) * ROWS, h * LANES : (h + 1) * LANES]

    def grad_rows(p, k, d):
        out = nn(hid_c[k % 2].reshape(CF, T), d[:]).astype(BF16)
        for o in range(8):
            for h in range(2):
                for i in range(7):
                    grad[p % HELD, o % 2, h, o // 2, i * HALF : (i + 1) * HALF, :] = out[
                        o * OWN + h * HALF : o * OWN + h * HALF + HALF, i * LANES : (i + 1) * LANES
                    ]

    def hidden_back(g, u, dp):
        s = sigmoid(g)
        act = g * s
        return act, (dp * u * (s + act * (1.0 - s))).astype(BF16), (dp * act).astype(BF16)

    def rows_of(r, n=RB):
        return pl.ds(pl.multiple_of(r * n, n), n)

    def forward(acc):
        weights_of(0, start)
        halves = [pltpu.make_async_copy(x.at[rows_of(r)], xv.at[rows_of(r)], load_sem.at[r]) for r in range(NRB)]
        for copy in halves:
            copy.start()
        load_dy.start()

        def normed_input(r):
            halves[r].wait()
            wide = xv[rows_of(r), :].astype(F32)
            av[rows_of(r), :] = (wide * norm_scale(wide)).astype(BF16)

        def step(j, first):
            b = j % 2
            weights_of(j + 1, start)
            weights_of(j, wait)
            if not first:

                @pl.when(j > 1)
                def _():
                    keep_hidden0(j - 2).wait()

            for r in range(NRB):
                rows = rows_of(r)
                a = av[rows, :]
                g = nn(a, wgj[b])
                u = nn(a, wuj[b])
                hid = (g * sigmoid(g) * u).astype(BF16)
                hid_c[b, :, :, rows] = hid.T.reshape(8, OWN, RB)
                y = nn(hid, wdj[b])
                acc[rows, :] = y if first else acc[rows, :] + y

            keep_hidden0(j).start()

        for r in range(NRB):
            normed_input(r)
        step(0, True)

        @pl.loop(1, STEPS)
        def _(j):
            step(j, False)

        @pl.loop(0, NRB)
        def _(r):
            rows = rows_of(r)
            y = acc[rows, :].astype(BF16).astype(F32)
            h = (xv[rows, :].astype(F32) + y).astype(BF16)
            xv[rows, :] = h
            wide = h.astype(F32)
            av[rows, :] = (wide * norm_scale(wide)).astype(BF16)

        keep_hidden0(STEPS - 2).wait()
        load_dy.wait()

    def first_layer(t):
        j = t // 4
        b = (j + 1) % 2

        @pl.when(t % 4 == 0)
        def _():
            weights_of(STEPS + j + 1, start)
            weights_of(STEPS + j, wait)

            @pl.when(j > 0)
            def _():
                keep_hidden(j - 1).wait()
                for copy in keep_d(j - 1):
                    copy.wait()

        @pl.when(t % 4 < 2)
        def _():
            rows = rows_of(t % 4)
            a = av[rows, :]
            at[:, rows] = a.T
            g = nn(a, wgj[b])
            u = nn(a, wuj[b])
            dp = nt(dyv[rows, :], wdj[b]).astype(BF16).astype(F32)
            act, dgr, dur = hidden_back(g, u, dp)
            hid_c[1, :, :, rows] = (act * u).astype(BF16).T.reshape(8, OWN, RB)
            dg[rows, :] = dgr
            du[rows, :] = dur

        @pl.when(t % 4 == 2)
        def _():
            keep_hidden(j).start()
            for copy in keep_d(j):
                copy.start()
            grad_columns(2 * j, dg)

        @pl.when(t % 4 == 3)
        def _():
            grad_columns(2 * j + 1, du)

            @pl.when(j == STEPS - 1)
            def _():
                keep_hidden(STEPS - 1).wait()
                for copy in keep_d(STEPS - 1):
                    copy.wait()
                keep_hidden0(STEPS - 1).wait()
                hidden_of(hid1_t, 0, True)

    def between(t, wgl, wul, dgb, dub):
        k = (t - 36) // 2
        block = lambda i: (
            pltpu.make_async_copy(dg1.at[rows_of(i, CF)], dgb, da_sem.at[2]),
            pltpu.make_async_copy(du1.at[rows_of(i, CF)], dub, da_sem.at[3]),
            pltpu.make_async_copy(x.at[rows_of(i, CF)], av.at[rows_of(i, CF)], da_sem.at[4]),
        )
        weights = (
            pltpu.make_async_copy(wg.at[1], wgl, da_sem.at[0]),
            pltpu.make_async_copy(wu.at[1], wul, da_sem.at[1]),
        )

        @pl.when(t == 36)
        def _():
            for copy in (*weights, *block(0)):
                copy.start()

        @pl.when(t == 38)
        def _():
            for copy in weights:
                copy.wait()

        @pl.when((k > 0) & (t % 2 == 0))
        def _():
            for copy in block(k - 1):
                copy.wait()
            by_g = nt(wgl[:], dgb[:])
            by_u = nt(wul[:], dub[:])
            da = by_g.astype(BF16).astype(F32) + by_u.astype(BF16).astype(F32)
            da = da.astype(BF16).T.astype(F32)
            rows = rows_of(k - 1, CF)
            wide = xv[rows, :].astype(F32)
            scale = norm_scale(wide)
            along = jnp.sum(da * wide, -1, keepdims=True) * (scale * scale * scale) * (-1.0 / D)
            back = (da * scale + wide * along).astype(BF16)
            xv[rows, :] = (dyv[rows, :].astype(F32) + back.astype(F32)).astype(BF16)
            wide = av[rows, :].astype(F32)
            a = (wide * norm_scale(wide)).astype(BF16)
            av[rows, :] = a
            at[:, rows] = a.T

            @pl.when(k < 8)
            def _():
                for copy in block(k):
                    copy.start()

        @pl.when(t % 2 == 1)
        def _():
            @pl.when(k < 8)
            def _():
                hidden_of(hid1_t, k + 1, True)

            hidden_of(hid1_t, k, False)
            grad_rows(18 + k, k, dyv)

    def last_layer(t):
        j = (t - 54) // 4
        b = j % 2
        turn = (t - 54) % 4
        k = (t - 90) // 2

        @pl.when((t < 90) & (turn == 0))
        def _():
            weights_of(2 * STEPS + j + 1, start)
            weights_of(2 * STEPS + j, wait)

        @pl.when((t < 90) & (turn < 2))
        def _():
            rows = rows_of(turn)
            a = av[rows, :]
            g = nn(a, wgj[b])
            u = nn(a, wuj[b])
            dp = nt(xv[rows, :], wdj[b]).astype(BF16).astype(F32)
            _, dgr, dur = hidden_back(g, u, dp)
            dg[rows, :] = dgr
            du[rows, :] = dur

        @pl.when((t < 90) & (turn == 2))
        def _():
            grad_columns(PER_LAYER + 2 * j, dg)

        @pl.when((t < 90) & (turn == 3))
        def _():
            grad_columns(PER_LAYER + 2 * j + 1, du)

            @pl.when(t == 89)
            def _():
                hidden_of(hid0_t, 0, True)

        @pl.when((t >= 90) & (t < Q) & (t % 2 == 1))
        def _():
            @pl.when(k < 8)
            def _():
                hidden_of(hid0_t, k + 1, True)

            hidden_of(hid0_t, k, False)
            grad_rows(PER_LAYER + 18 + k, k, xv)

    def chunk_after(t):
        n = t % 54
        pair = n < 36
        return (t < Q) & jnp.where(pair, n % 4 >= 2, n % 2 == 1), (t // 54) * PER_LAYER + jnp.where(
            pair, 2 * (n // 4) + n % 2, n // 2
        )

    f32 = lambda t: t.astype(F32)

    def sums(t):
        q = t - 3

        @pl.when(valid(q) & (q % 2 == 0))
        def _():
            to_partner(q // 2).wait_recv()

        qr = t - 3 - LAG * z
        ql = t - 3 - LAG * (3 - z)

        def own(q, to):
            e = (q // 2) % HELD
            return f32(grad[e, c, q % 2, to]) + f32(pin[e, q % 2, to])

        for zz in range(4):

            @pl.when(z == zz)
            def _():
                @pl.when(valid(qr))
                def _():
                    if zz > 0:
                        sum_right(qr, zz - 1).wait_recv()
                    if zz < 3:

                        @pl.when(qr >= OUT)
                        def _():
                            sum_right(qr - OUT, zz).wait_send()

                        for to in range(zz + 1, 4):
                            total = own(qr, to)
                            if zz > 0:
                                total = total + f32(sums_in[qr % RING, to - zz])
                            rout[qr % OUT, to - 1] = total.astype(BF16)
                        sum_right(qr, zz).start()

                @pl.when(valid(ql))
                def _():
                    if zz < 3:
                        sum_left(ql, zz + 1).wait_recv()
                    if zz > 0:

                        @pl.when(ql >= OUT)
                        def _():
                            sum_left(ql - OUT, zz).wait_send()

                        for to in range(zz):
                            total = own(ql, to)
                            if zz < 3:
                                total = total + f32(sums_in[ql % RING, 4 - zz + to])
                            lout[ql % OUT, to] = total.astype(BF16)
                        sum_left(ql, zz).start()

    def optimizer(t):
        q = t - 3 - LAG * jnp.maximum(z, 3 - z)

        @pl.when((q >= 1) & (q <= Q))
        def _():
            keep_moments(q - 1, wait)

        @pl.when(valid(q + 1))
        def _():
            moments(q + 1, start)

        @pl.when(valid(q))
        def _():
            e, h = (q // 2) % HELD, q % 2
            gfin[:] = f32(grad[e, c, h, z]) + f32(pin[e, h, z])

            @pl.when(z > 0)
            def _():
                gfin[:] += f32(sums_in[q % RING, 0])

            @pl.when(z < 3)
            def _():
                gfin[:] += f32(sums_in[q % RING, 4])

            moments(q, wait)
            layer, n, _, cols, rows = place(q)

            @pl.when((n < 18) & (n % 2 == 0))
            def _():
                g = f32(gfin[:].astype(BF16))
                news[q % RING, z], nmg[layer, :, cols], nvg[layer, :, cols] = adamw(f32(wb[h]), mb[h], vb[h], g)

            @pl.when((n < 18) & (n % 2 == 1))
            def _():
                g = f32(gfin[:].astype(BF16))
                news[q % RING, z], nmu[layer, :, cols], vb[h] = adamw(f32(wb[h]), mb[h], vb[h], g)

            @pl.when(n >= 18)
            def _():
                for i in range(7):
                    lanes = slice(i * LANES, (i + 1) * LANES)
                    part = slice(i * HALF, (i + 1) * HALF)
                    g = f32(gfin[part, :].astype(BF16))
                    news[q % RING, z, part, :], nmd[layer, rows, lanes], vbd[h, :, lanes] = adamw(
                        f32(wbd[h, :, lanes]), mbd[h, :, lanes], vbd[h, :, lanes], g
                    )

            keep_moments(q, start)

    def send(copy, q, frm):
        @pl.when(q >= SENDS)
        def _():
            copy(q - SENDS, frm).wait_send()

        copy(q, frm).start()

    def spread(t):
        for zz in range(4):

            @pl.when(z == zz)
            def _():
                q = t - 4 - LAG * max(zz, 3 - zz)

                @pl.when(valid(q))
                def _():
                    if zz < 3:
                        send(own_right, q, zz)
                    if zz > 0:
                        send(own_left, q, zz)

                if zz in (1, 2):
                    near, far = t - 4 - 4 * LAG, t - 4 - 5 * LAG
                    qr, ql = (near, far) if zz == 1 else (far, near)

                    @pl.when(valid(qr))
                    def _():
                        own_right(qr, zz - 1).wait_recv()
                        if zz == 2:
                            on_right(qr, 1).wait_recv()
                        send(on_right, qr, zz)

                    @pl.when(valid(ql))
                    def _():
                        own_left(ql, zz + 1).wait_recv()
                        if zz == 1:
                            on_left(ql, 2).wait_recv()
                        send(on_left, ql, zz)
                else:
                    q = t - SPREAD

                    @pl.when(valid(q))
                    def _():
                        if zz == 3:
                            own_right(q, 2).wait_recv()
                            on_right(q, 2).wait_recv()
                        else:
                            own_left(q, 1).wait_recv()
                            on_left(q, 1).wait_recv()

        q = t - SPREAD

        @pl.when(valid(q))
        def _():
            @pl.when(q >= 2)
            def _():
                new_partner(q - 2, c).wait_send()
                keep_new(q - 2).wait()

            new_partner(q, c).start()
            keep_new(q).start()

        @pl.when(valid(q - 2))
        def _():
            new_partner(q - 2, 1 - c).wait_recv()

    def last_waits():
        for i in range(2):
            to_partner(CHUNKS - 2 + i).wait_send()
            keep_new(Q - 2 + i).wait()
            new_partner(Q - 2 + i, c).wait_send()
        for zz in range(4):

            @pl.when(z == zz)
            def _():
                for q in range(Q - SENDS, Q):
                    if zz < 3:
                        if q >= Q - OUT:
                            sum_right(q, zz).wait_send()
                        own_right(q, zz).wait_send()
                    if zz > 0:
                        if q >= Q - OUT:
                            sum_left(q, zz).wait_send()
                        own_left(q, zz).wait_send()
                    if zz in (1, 2):
                        on_right(q, zz).wait_send()
                        on_left(q, zz).wait_send()

    def slots(first, last, compute):
        @pl.loop(first, last)
        def _(t):
            compute(t)
            ready, p = chunk_after(t)

            @pl.when(ready)
            def _():
                @pl.when(p >= 2)
                def _():
                    to_partner(p - 2).wait_send()

                to_partner(p).start()

            sums(t)
            optimizer(t)
            spread(t)

    pl.run_scoped(forward, pltpu.VMEM((T, D), F32))

    @pl.when((z == 0) | (z == 3))
    def _():
        pl.semaphore_wait(bar, 2)

    @pl.when((z > 0) & (z < 3))
    def _():
        pl.semaphore_wait(bar, 3)

    slots(0, 36, first_layer)
    pl.run_scoped(
        lambda *bufs: slots(36, 54, lambda t: between(t, *bufs)),
        pltpu.VMEM((D, FF), BF16), pltpu.VMEM((D, FF), BF16), pltpu.VMEM((CF, FF), BF16), pltpu.VMEM((CF, FF), BF16),
    )
    slots(54, LAST, last_layer)
    last_waits()


def train(*operands):
    vm = pltpu.VMEM
    dma = pltpu.SemaphoreType.DMA
    any_, inside = pl.BlockSpec(memory_space=pl.ANY), pl.BlockSpec(memory_space=vm)
    shape = jax.ShapeDtypeStruct
    out_shape = [
        shape((CHUNKS, 2, 2, 4, ROWS, LANES), BF16), *[shape(t.shape, F32) for t in operands[3:9]],
        shape((72, OWN, T), BF16), shape((72, OWN, T), BF16),
        shape((T, FF), BF16), shape((T, FF), BF16),
    ]
    return pl.pallas_call(
        train_kernel,
        in_specs=[any_] * len(operands),
        out_specs=[any_, *[inside] * 4, *[any_] * (len(out_shape) - 5)],
        out_shape=out_shape,
        scratch_shapes=[
            vm((T, D), BF16), vm((T, D), BF16), vm((T, D), BF16), vm((D, T), BF16),
            vm((T, CF), BF16), vm((T, CF), BF16),
            vm((2, D, CF), BF16), vm((2, D, CF), BF16), vm((2, CF, D), BF16),
            vm((2, 8, OWN, T), BF16),
            vm((HELD, 2, 2, 4, ROWS, LANES), BF16), vm((HELD, 2, 4, ROWS, LANES), BF16),
            vm((RING, 5, ROWS, LANES), BF16),
            vm((OUT, 3, ROWS, LANES), BF16), vm((OUT, 3, ROWS, LANES), BF16),
            vm((RING, 4, ROWS, LANES), BF16), vm((ROWS, LANES), F32),
            vm((2, ROWS, LANES), F32), vm((2, ROWS, LANES), F32), vm((2, ROWS, LANES), BF16),
            vm((2, HALF, D), F32), vm((2, HALF, D), F32), vm((2, HALF, D), BF16),
            dma((3,)), dma((2, 3)), dma, dma((2,)), dma((2,)), dma((5,)),
            dma((2,)), dma((HELD,)), dma((SENDS,)), dma((RING,)), dma((SENDS,)), dma((RING,)),
            dma((SENDS,)), dma((RING,)), dma((SENDS,)), dma((RING,)), dma((SENDS,)), dma((RING,)),
            dma((SENDS,)), dma((RING,)), dma((SENDS,)), dma((RING,)), dma((SENDS,)), dma((2,)), dma((2, 3)),
        ],
        compiler_params=pltpu.CompilerParams(
            collective_id=0, has_side_effects=True, vmem_limit_bytes=VMEM_LIMIT
        ),
        name="train",
    )(*operands)


AHEAD = 12


def finish_kernel(
    wt, mg, mu, md, vg, vu, vd, owg, owu, owd, omg, omu, omd, ovg, ovu, ovd,
    wv, vuv, vdv, columns, rows, w_sem, in_sem, out_sem, col_sem, row_sem,
):
    moments = ((mg, omg), (mu, omu), (md, omd), (vg, ovg), (vuv, ovu), (vdv, ovd))
    pieces = [(i, layer) for layer in (1, 0) for i in range(6)]

    def take(layer):
        return [pltpu.make_async_copy(a.at[layer], b.at[layer], in_sem.at[i, layer]) for i, (a, b) in enumerate(((vu, vuv), (vd, vdv)))]

    def give(i, layer):
        return pltpu.make_async_copy(moments[i][0].at[layer], moments[i][1].at[layer], out_sem.at[i, layer])

    def chunk(p):
        return pltpu.make_async_copy(wt.at[p], wv.at[p % (AHEAD + 1)], w_sem.at[p % (AHEAD + 1)])

    def columns_out(out, layer, j, b):
        return pltpu.make_async_copy(columns.at[b], out.at[layer, :, pl.ds(pl.multiple_of(j * CF, CF), CF)], col_sem.at[b])

    def rows_out(layer, k, b):
        return pltpu.make_async_copy(rows.at[b], owd.at[layer, :, pl.ds(pl.multiple_of(k * OWN, OWN), OWN), :], row_sem.at[b])

    for p in range(AHEAD):
        chunk(p).start()

    def chunk_in(p):
        @pl.when(p + AHEAD < CHUNKS)
        def _():
            chunk(p + AHEAD).start()

        chunk(p).wait()

    for part in range(18):
        layer, base, n0 = 1 - part // 9, part // 9 * PER_LAYER, part % 9 * 3

        @pl.loop(0, 3)
        def _(i):
            n = n0 + i
            p = base + n
            chunk_in(p)
            e = p % (AHEAD + 1)
            if n0 < 18:
                b = n % 4

                @pl.when((n >= 4) | (base > 0))
                def _():
                    columns_out(owg, layer, 0, b).wait()

                for o in range(8):
                    for h in range(2):
                        columns[b, o * ROWS : (o + 1) * ROWS, h * LANES : (h + 1) * LANES] = wv[e, o % 2, h, o // 2]

                @pl.when(n % 2 == 0)
                def _():
                    columns_out(owg, layer, n // 2, b).start()

                @pl.when(n % 2 == 1)
                def _():
                    columns_out(owu, layer, n // 2, b).start()
            else:
                k = n - 18
                b = k % 4

                @pl.when((k >= 4) | (base > 0))
                def _():
                    rows_out(layer, 0, b).wait()

                for o in range(8):
                    for h in range(2):
                        for c in range(7):
                            rows[b, o, h * HALF : (h + 1) * HALF, c * LANES : (c + 1) * LANES] = wv[
                                e, o % 2, h, o // 2, c * HALF : (c + 1) * HALF, :
                            ]
                rows_out(layer, k, b).start()

        if part < 12:
            piece, side = pieces[part], part % 6
            if side == 0:
                for copy in take(piece[1]):
                    copy.start()
            if side == 4:
                for copy in take(piece[1]):
                    copy.wait()
            give(*piece).start()

    for b in range(4):
        columns_out(owg, 0, 0, b).wait()
        rows_out(0, 0, b).wait()
    for piece in pieces:
        give(*piece).wait()


def finish(wtmp, *moments):
    vm, dma = pltpu.VMEM, pltpu.SemaphoreType.DMA
    any_, inside = pl.BlockSpec(memory_space=pl.ANY), pl.BlockSpec(memory_space=vm)
    out = pl.pallas_call(
        finish_kernel,
        in_specs=[any_, *[inside] * 4, any_, any_],
        out_specs=[any_] * 9,
        out_shape=[
            jax.ShapeDtypeStruct((2, D, FF), BF16), jax.ShapeDtypeStruct((2, D, FF), BF16),
            jax.ShapeDtypeStruct((2, 8, 288, D), BF16),
            *[jax.ShapeDtypeStruct(t.shape, F32) for t in moments],
        ],
        scratch_shapes=[
            vm((AHEAD + 1, *wtmp.shape[1:]), BF16), vm(moments[4].shape, F32), vm(moments[5].shape, F32),
            vm((4, D, CF), BF16), vm((4, 8, OWN, D), BF16),
            dma((AHEAD + 1,)), dma((2, 2)), dma((6, 2)), dma((4,)), dma((4,)),
        ],
        compiler_params=pltpu.CompilerParams(vmem_limit_bytes=48000000),
        name="finish",
    )(wtmp, *moments)
    return (out[0], out[1], out[2].reshape(2, FF, D), *out[3:])


def solution(mesh):
    def step(x, dy, wg, wu, wd, *moments):
        out = train(wg, wu, wd, *moments, x[0], dy[0])
        return finish(*out[:7])

    seq, whole, rows = P(("rep", "dp")), P(), P(None, "dp")
    return jax.shard_map(
        step, mesh=mesh,
        in_specs=(seq, seq, *[whole] * 3, *[rows] * 6),
        out_specs=(*[P("rep")] * 3, *[P("rep", "dp")] * 6),
        check_vma=False,
    )
```

```python
import jax
import jax.numpy as jnp
from jax import lax
from jax.experimental import pallas as pl
from jax.experimental.pallas import tpu as pltpu
from jax.sharding import PartitionSpec as P

MESH = pl.DeviceIdType.MESH
F32, BF16 = jnp.float32, jnp.bfloat16
T, D, FF = 2048, 896, 2304
CF = 256
STEPS = FF // CF
RB = 1024
NRB = T // RB
LANES = 128
HALF = 16
OWN = 32
ROWS = 112
PER_LAYER = 27
CHUNKS = 2 * PER_LAYER
Q = 2 * CHUNKS
LAG = 2
HELD = 8
RING = 2 * HELD
SENDS = 4
OUT = 3
SPREAD = 4 + 6 * LAG
LAST = Q + SPREAD + 3
VMEM_LIMIT = 48000000


def nt(a, b):
    return lax.dot_general(a, b, (((1,), (1,)), ((), ())), preferred_element_type=F32)


def nn(a, b):
    return jnp.dot(a, b, preferred_element_type=F32)


def norm_scale(wide):
    return lax.rsqrt(jnp.mean(wide * wide, -1, keepdims=True) + 1e-6)


def sigmoid(g):
    return 1.0 / (1.0 + jnp.exp(-g))


def train_kernel(
    wg, wu, wd, mg, mu, md, vg, vu, vd, x, dy,
    wtmp, nmg, nmu, nmd, nvg, nvu, nvd, hid0_t, hid1_t, dg1, du1,
    xv, dyv, av, at, dg, du, wgj, wuj, wdj, hid_c,
    grad, pin, sums_in, rout, lout, news, gfin, mb, vb, wb, mbd, vbd, wbd,
    load_sem, w_sem, hw_sem, hc_sem, d_sem, da_sem,
    p_send, p_recv, r_send, r_recv, l_send, l_recv,
    or_send, or_recv, ol_send, ol_recv, ar_send, ar_recv, al_send, al_recv, ap_send, ap_recv, wo_sem, mo_sem, ad_sem,
):
    rep, me = lax.axis_index("rep"), lax.axis_index("dp")
    z, c = me // 2, me % 2
    partner = (rep, z * 2 + (1 - c))
    right = (rep, jnp.minimum(z + 1, 3) * 2 + c)
    left = (rep, jnp.maximum(z - 1, 0) * 2 + c)

    bar = pltpu.get_barrier_semaphore()
    pl.semaphore_signal(bar, inc=1, device_id=partner, device_id_type=MESH)

    @pl.when(z < 3)
    def _():
        pl.semaphore_signal(bar, inc=1, device_id=right, device_id_type=MESH)

    @pl.when(z > 0)
    def _():
        pl.semaphore_signal(bar, inc=1, device_id=left, device_id_type=MESH)

    valid = lambda q: (q >= 0) & (q < Q)

    def remote(src, dst, send, recv, to):
        return pltpu.make_async_remote_copy(
            src_ref=src, dst_ref=dst, send_sem=send, recv_sem=recv, device_id=to, device_id_type=MESH
        )

    def to_partner(p):
        e = p % HELD
        return remote(grad.at[e, 1 - c], pin.at[e], p_send.at[p % 2], p_recv.at[e], partner)

    def sum_right(q, frm):
        part = pl.ds(frm, 3 - frm)
        there = pl.ds(0, 3 - frm)
        return remote(rout.at[q % OUT, part], sums_in.at[q % RING, there], r_send.at[q % OUT], r_recv.at[q % RING], right)

    def sum_left(q, frm):
        part = pl.ds(0, frm)
        there = pl.ds(5 - frm, frm)
        return remote(lout.at[q % OUT, part], sums_in.at[q % RING, there], l_send.at[q % OUT], l_recv.at[q % RING], left)

    def own_right(q, frm):
        here = news.at[q % RING, pl.ds(frm, 1)]
        return remote(here, here, or_send.at[q % SENDS], or_recv.at[q % RING], right)

    def own_left(q, frm):
        here = news.at[q % RING, pl.ds(frm, 1)]
        return remote(here, here, ol_send.at[q % SENDS], ol_recv.at[q % RING], left)

    def on_right(q, frm):
        here = news.at[q % RING, pl.ds(0, frm)]
        return remote(here, here, ar_send.at[q % SENDS], ar_recv.at[q % RING], right)

    def on_left(q, frm):
        here = news.at[q % RING, pl.ds(frm + 1, 3 - frm)]
        return remote(here, here, al_send.at[q % SENDS], al_recv.at[q % RING], left)

    def new_partner(q, core):
        return remote(
            news.at[q % RING], wtmp.at[q // 2, core, q % 2], ap_send.at[q % SENDS], ap_recv.at[q % RING], partner
        )

    def keep_new(q):
        return pltpu.make_async_copy(news.at[q % RING], wtmp.at[q // 2, c, q % 2], wo_sem.at[q % SENDS])

    def place(q):
        p, s = q // 2, q % 2
        n = p % PER_LAYER
        cols = pl.ds(pl.multiple_of((n // 2) * CF + s * LANES, LANES), LANES)
        rows = pl.ds(pl.multiple_of(jnp.maximum(n - 18, 0) * OWN + s * HALF, HALF), HALF)
        return jnp.where(p < PER_LAYER, 1, 0), n, s, cols, rows

    def moments(q, act):
        layer, n, s, cols, rows = place(q)
        for which, (m, v, w) in enumerate(((mg, vg, wg), (mu, vu, wu))):

            @pl.when((n < 18) & (n % 2 == which))
            def _():
                own = pl.ds(pl.multiple_of(me * ROWS, HALF), ROWS)
                act(pltpu.make_async_copy(m.at[layer, :, cols], mb.at[s], ad_sem.at[s, 0]))
                act(pltpu.make_async_copy(v.at[layer, :, cols], vb.at[s], ad_sem.at[s, 1]))
                act(pltpu.make_async_copy(w.at[layer, own, cols], wb.at[s], ad_sem.at[s, 2]))

        @pl.when(n >= 18)
        def _():
            own = pl.ds(pl.multiple_of(me * 288 + (n - 18) * OWN + s * HALF, HALF), HALF)
            act(pltpu.make_async_copy(md.at[layer, rows, :], mbd.at[s], ad_sem.at[s, 0]))
            act(pltpu.make_async_copy(vd.at[layer, rows, :], vbd.at[s], ad_sem.at[s, 1]))
            act(pltpu.make_async_copy(wd.at[layer, own, :], wbd.at[s], ad_sem.at[s, 2]))

    def keep_moments(q, act):
        layer, n, s, cols, rows = place(q)

        @pl.when((n < 18) & (n % 2 == 1))
        def _():
            act(pltpu.make_async_copy(vb.at[s], nvu.at[layer, :, cols], mo_sem.at[s]))

        @pl.when(n >= 18)
        def _():
            act(pltpu.make_async_copy(vbd.at[s], nvd.at[layer, rows, :], mo_sem.at[s]))

    def adamw(w, m, v, g):
        m = 0.9 * m + 0.1 * g
        v = 0.95 * v + 0.05 * g * g
        step = m * lax.rsqrt(v + 1e-8) + 0.1 * w
        return (w - 0.02 * step).astype(BF16), m, v

    def weights_of(n, act):
        s = n % 2
        cols = pl.ds(pl.multiple_of((n % STEPS) * CF, CF), CF)
        layer = jnp.where((n >= STEPS) & (n < 2 * STEPS), 1, 0)

        @pl.when(n < 3 * STEPS)
        def _():
            act(pltpu.make_async_copy(wg.at[layer, :, cols], wgj.at[s], w_sem.at[s, 0]))
            act(pltpu.make_async_copy(wu.at[layer, :, cols], wuj.at[s], w_sem.at[s, 1]))
            act(pltpu.make_async_copy(wd.at[layer, cols, :], wdj.at[s], w_sem.at[s, 2]))

    def keep_hidden0(j):
        return pltpu.make_async_copy(hid_c.at[j % 2], hid0_t.at[pl.ds(j * 8, 8)], hc_sem.at[j % 2])

    def keep_hidden(j):
        return pltpu.make_async_copy(hid_c.at[1], hid1_t.at[pl.ds(j * 8, 8)], hw_sem)

    def keep_d(j):
        cols = pl.ds(pl.multiple_of(j * CF, CF), CF)
        return (
            pltpu.make_async_copy(dg, dg1.at[:, cols], d_sem.at[0]),
            pltpu.make_async_copy(du, du1.at[:, cols], d_sem.at[1]),
        )

    def hidden_of(src, k, start):
        s = k % 2
        if start:
            for o in range(8):
                pltpu.make_async_copy(src.at[o * 9 + k], hid_c.at[s, o], hc_sem.at[s]).start()
        else:
            pltpu.make_async_copy(src.at[pl.ds(0, 8)], hid_c.at[s], hc_sem.at[s]).wait()

    load_dy = pltpu.make_async_copy(dy, dyv, load_sem.at[2])

    start = lambda copy: copy.start()
    wait = lambda copy: copy.wait()

    def grad_columns(p, d):
        out = nn(at[:], d[:]).astype(BF16)
        for o in range(8):
            for h in range(2):
                grad[p % HELD, o % 2, h, o // 2] = out[o * ROWS : (o + 1) * ROWS, h * LANES : (h + 1) * LANES]

    def grad_rows(p, k, d):
        out = nn(hid_c[k % 2].reshape(CF, T), d[:]).astype(BF16)
        for o in range(8):
            for h in range(2):
                for i in range(7):
                    grad[p % HELD, o % 2, h, o // 2, i * HALF : (i + 1) * HALF, :] = out[
                        o * OWN + h * HALF : o * OWN + h * HALF + HALF, i * LANES : (i + 1) * LANES
                    ]

    def hidden_back(g, u, dp):
        s = sigmoid(g)
        act = g * s
        return act, (dp * u * (s + act * (1.0 - s))).astype(BF16), (dp * act).astype(BF16)

    def rows_of(r, n=RB):
        return pl.ds(pl.multiple_of(r * n, n), n)

    def forward(acc):
        weights_of(0, start)
        halves = [pltpu.make_async_copy(x.at[rows_of(r)], xv.at[rows_of(r)], load_sem.at[r]) for r in range(NRB)]
        for copy in halves:
            copy.start()
        load_dy.start()

        def normed_input(r):
            halves[r].wait()
            wide = xv[rows_of(r), :].astype(F32)
            av[rows_of(r), :] = (wide * norm_scale(wide)).astype(BF16)

        def step(j, first):
            b = j % 2
            weights_of(j + 1, start)
            weights_of(j, wait)
            if not first:

                @pl.when(j > 1)
                def _():
                    keep_hidden0(j - 2).wait()

            for r in range(NRB):
                rows = rows_of(r)
                a = av[rows, :]
                g = nn(a, wgj[b])
                u = nn(a, wuj[b])
                hid = (g * sigmoid(g) * u).astype(BF16)
                hid_c[b, :, :, rows] = hid.T.reshape(8, OWN, RB)
                y = nn(hid, wdj[b])
                acc[rows, :] = y if first else acc[rows, :] + y

            keep_hidden0(j).start()

        for r in range(NRB):
            normed_input(r)
        step(0, True)

        @pl.loop(1, STEPS)
        def _(j):
            step(j, False)

        @pl.loop(0, NRB)
        def _(r):
            rows = rows_of(r)
            y = acc[rows, :].astype(BF16).astype(F32)
            h = (xv[rows, :].astype(F32) + y).astype(BF16)
            xv[rows, :] = h
            wide = h.astype(F32)
            av[rows, :] = (wide * norm_scale(wide)).astype(BF16)

        keep_hidden0(STEPS - 2).wait()
        load_dy.wait()

    def first_layer(t):
        j = t // 4
        b = (j + 1) % 2

        @pl.when(t % 4 == 0)
        def _():
            weights_of(STEPS + j + 1, start)
            weights_of(STEPS + j, wait)

            @pl.when(j > 0)
            def _():
                keep_hidden(j - 1).wait()
                for copy in keep_d(j - 1):
                    copy.wait()

        @pl.when(t % 4 < 2)
        def _():
            rows = rows_of(t % 4)
            a = av[rows, :]
            at[:, rows] = a.T
            g = nn(a, wgj[b])
            u = nn(a, wuj[b])
            dp = nt(dyv[rows, :], wdj[b]).astype(BF16).astype(F32)
            act, dgr, dur = hidden_back(g, u, dp)
            hid_c[1, :, :, rows] = (act * u).astype(BF16).T.reshape(8, OWN, RB)
            dg[rows, :] = dgr
            du[rows, :] = dur

        @pl.when(t % 4 == 2)
        def _():
            keep_hidden(j).start()
            for copy in keep_d(j):
                copy.start()
            grad_columns(2 * j, dg)

        @pl.when(t % 4 == 3)
        def _():
            grad_columns(2 * j + 1, du)

            @pl.when(j == STEPS - 1)
            def _():
                keep_hidden(STEPS - 1).wait()
                for copy in keep_d(STEPS - 1):
                    copy.wait()
                keep_hidden0(STEPS - 1).wait()
                hidden_of(hid1_t, 0, True)

    def between(t, wgl, wul, dgb, dub):
        k = (t - 36) // 2
        block = lambda i: (
            pltpu.make_async_copy(dg1.at[rows_of(i, CF)], dgb, da_sem.at[2]),
            pltpu.make_async_copy(du1.at[rows_of(i, CF)], dub, da_sem.at[3]),
            pltpu.make_async_copy(x.at[rows_of(i, CF)], av.at[rows_of(i, CF)], da_sem.at[4]),
        )
        weights = (
            pltpu.make_async_copy(wg.at[1], wgl, da_sem.at[0]),
            pltpu.make_async_copy(wu.at[1], wul, da_sem.at[1]),
        )

        @pl.when(t == 36)
        def _():
            for copy in (*weights, *block(0)):
                copy.start()

        @pl.when(t == 38)
        def _():
            for copy in weights:
                copy.wait()

        @pl.when((k > 0) & (t % 2 == 0))
        def _():
            for copy in block(k - 1):
                copy.wait()
            by_g = nt(wgl[:], dgb[:])
            by_u = nt(wul[:], dub[:])
            da = by_g.astype(BF16).astype(F32) + by_u.astype(BF16).astype(F32)
            da = da.astype(BF16).T.astype(F32)
            rows = rows_of(k - 1, CF)
            wide = xv[rows, :].astype(F32)
            scale = norm_scale(wide)
            along = jnp.sum(da * wide, -1, keepdims=True) * (scale * scale * scale) * (-1.0 / D)
            back = (da * scale + wide * along).astype(BF16)
            xv[rows, :] = (dyv[rows, :].astype(F32) + back.astype(F32)).astype(BF16)
            wide = av[rows, :].astype(F32)
            a = (wide * norm_scale(wide)).astype(BF16)
            av[rows, :] = a
            at[:, rows] = a.T

            @pl.when(k < 8)
            def _():
                for copy in block(k):
                    copy.start()

        @pl.when(t % 2 == 1)
        def _():
            @pl.when(k < 8)
            def _():
                hidden_of(hid1_t, k + 1, True)

            hidden_of(hid1_t, k, False)
            grad_rows(18 + k, k, dyv)

    def last_layer(t):
        j = (t - 54) // 4
        b = j % 2
        turn = (t - 54) % 4
        k = (t - 90) // 2

        @pl.when((t < 90) & (turn == 0))
        def _():
            weights_of(2 * STEPS + j + 1, start)
            weights_of(2 * STEPS + j, wait)

        @pl.when((t < 90) & (turn < 2))
        def _():
            rows = rows_of(turn)
            a = av[rows, :]
            g = nn(a, wgj[b])
            u = nn(a, wuj[b])
            dp = nt(xv[rows, :], wdj[b]).astype(BF16).astype(F32)
            _, dgr, dur = hidden_back(g, u, dp)
            dg[rows, :] = dgr
            du[rows, :] = dur

        @pl.when((t < 90) & (turn == 2))
        def _():
            grad_columns(PER_LAYER + 2 * j, dg)

        @pl.when((t < 90) & (turn == 3))
        def _():
            grad_columns(PER_LAYER + 2 * j + 1, du)

            @pl.when(t == 89)
            def _():
                hidden_of(hid0_t, 0, True)

        @pl.when((t >= 90) & (t < Q) & (t % 2 == 1))
        def _():
            @pl.when(k < 8)
            def _():
                hidden_of(hid0_t, k + 1, True)

            hidden_of(hid0_t, k, False)
            grad_rows(PER_LAYER + 18 + k, k, xv)

    def chunk_after(t):
        n = t % 54
        pair = n < 36
        return (t < Q) & jnp.where(pair, n % 4 >= 2, n % 2 == 1), (t // 54) * PER_LAYER + jnp.where(
            pair, 2 * (n // 4) + n % 2, n // 2
        )

    f32 = lambda t: t.astype(F32)

    def sums(t):
        q = t - 3

        @pl.when(valid(q) & (q % 2 == 0))
        def _():
            to_partner(q // 2).wait_recv()

        qr = t - 3 - LAG * z
        ql = t - 3 - LAG * (3 - z)

        def own(q, to):
            e = (q // 2) % HELD
            return f32(grad[e, c, q % 2, to]) + f32(pin[e, q % 2, to])

        for zz in range(4):

            @pl.when(z == zz)
            def _():
                @pl.when(valid(qr))
                def _():
                    if zz > 0:
                        sum_right(qr, zz - 1).wait_recv()
                    if zz < 3:

                        @pl.when(qr >= OUT)
                        def _():
                            sum_right(qr - OUT, zz).wait_send()

                        for to in range(zz + 1, 4):
                            total = own(qr, to)
                            if zz > 0:
                                total = total + f32(sums_in[qr % RING, to - zz])
                            rout[qr % OUT, to - 1] = total.astype(BF16)
                        sum_right(qr, zz).start()

                @pl.when(valid(ql))
                def _():
                    if zz < 3:
                        sum_left(ql, zz + 1).wait_recv()
                    if zz > 0:

                        @pl.when(ql >= OUT)
                        def _():
                            sum_left(ql - OUT, zz).wait_send()

                        for to in range(zz):
                            total = own(ql, to)
                            if zz < 3:
                                total = total + f32(sums_in[ql % RING, 4 - zz + to])
                            lout[ql % OUT, to] = total.astype(BF16)
                        sum_left(ql, zz).start()

    def optimizer(t):
        q = t - 3 - LAG * jnp.maximum(z, 3 - z)

        @pl.when((q >= 1) & (q <= Q))
        def _():
            keep_moments(q - 1, wait)

        @pl.when(valid(q + 1))
        def _():
            moments(q + 1, start)

        @pl.when(valid(q))
        def _():
            e, h = (q // 2) % HELD, q % 2
            gfin[:] = f32(grad[e, c, h, z]) + f32(pin[e, h, z])

            @pl.when(z > 0)
            def _():
                gfin[:] += f32(sums_in[q % RING, 0])

            @pl.when(z < 3)
            def _():
                gfin[:] += f32(sums_in[q % RING, 4])

            moments(q, wait)
            layer, n, _, cols, rows = place(q)

            @pl.when((n < 18) & (n % 2 == 0))
            def _():
                g = f32(gfin[:].astype(BF16))
                news[q % RING, z], nmg[layer, :, cols], nvg[layer, :, cols] = adamw(f32(wb[h]), mb[h], vb[h], g)

            @pl.when((n < 18) & (n % 2 == 1))
            def _():
                g = f32(gfin[:].astype(BF16))
                news[q % RING, z], nmu[layer, :, cols], vb[h] = adamw(f32(wb[h]), mb[h], vb[h], g)

            @pl.when(n >= 18)
            def _():
                for i in range(7):
                    lanes = slice(i * LANES, (i + 1) * LANES)
                    part = slice(i * HALF, (i + 1) * HALF)
                    g = f32(gfin[part, :].astype(BF16))
                    news[q % RING, z, part, :], nmd[layer, rows, lanes], vbd[h, :, lanes] = adamw(
                        f32(wbd[h, :, lanes]), mbd[h, :, lanes], vbd[h, :, lanes], g
                    )

            keep_moments(q, start)

    def send(copy, q, frm):
        @pl.when(q >= SENDS)
        def _():
            copy(q - SENDS, frm).wait_send()

        copy(q, frm).start()

    def spread(t):
        for zz in range(4):

            @pl.when(z == zz)
            def _():
                q = t - 4 - LAG * max(zz, 3 - zz)

                @pl.when(valid(q))
                def _():
                    if zz < 3:
                        send(own_right, q, zz)
                    if zz > 0:
                        send(own_left, q, zz)

                if zz in (1, 2):
                    near, far = t - 4 - 4 * LAG, t - 4 - 5 * LAG
                    qr, ql = (near, far) if zz == 1 else (far, near)

                    @pl.when(valid(qr))
                    def _():
                        own_right(qr, zz - 1).wait_recv()
                        if zz == 2:
                            on_right(qr, 1).wait_recv()
                        send(on_right, qr, zz)

                    @pl.when(valid(ql))
                    def _():
                        own_left(ql, zz + 1).wait_recv()
                        if zz == 1:
                            on_left(ql, 2).wait_recv()
                        send(on_left, ql, zz)
                else:
                    q = t - SPREAD

                    @pl.when(valid(q))
                    def _():
                        if zz == 3:
                            own_right(q, 2).wait_recv()
                            on_right(q, 2).wait_recv()
                        else:
                            own_left(q, 1).wait_recv()
                            on_left(q, 1).wait_recv()

        q = t - SPREAD

        @pl.when(valid(q))
        def _():
            @pl.when(q >= SENDS)
            def _():
                new_partner(q - SENDS, c).wait_send()
                keep_new(q - SENDS).wait()

            new_partner(q, c).start()
            keep_new(q).start()

        @pl.when(valid(q - 2))
        def _():
            new_partner(q - 2, 1 - c).wait_recv()

    def last_waits():
        for i in range(2):
            to_partner(CHUNKS - 2 + i).wait_send()
        for i in range(SENDS):
            keep_new(Q - SENDS + i).wait()
            new_partner(Q - SENDS + i, c).wait_send()
        for zz in range(4):

            @pl.when(z == zz)
            def _():
                for q in range(Q - SENDS, Q):
                    if zz < 3:
                        if q >= Q - OUT:
                            sum_right(q, zz).wait_send()
                        own_right(q, zz).wait_send()
                    if zz > 0:
                        if q >= Q - OUT:
                            sum_left(q, zz).wait_send()
                        own_left(q, zz).wait_send()
                    if zz in (1, 2):
                        on_right(q, zz).wait_send()
                        on_left(q, zz).wait_send()

    def slots(first, last, compute):
        @pl.loop(first, last)
        def _(t):
            compute(t)
            ready, p = chunk_after(t)

            @pl.when(ready)
            def _():
                @pl.when(p >= 2)
                def _():
                    to_partner(p - 2).wait_send()

                to_partner(p).start()

            sums(t)
            optimizer(t)
            spread(t)

    pl.run_scoped(forward, pltpu.VMEM((T, D), F32))

    @pl.when((z == 0) | (z == 3))
    def _():
        pl.semaphore_wait(bar, 2)

    @pl.when((z > 0) & (z < 3))
    def _():
        pl.semaphore_wait(bar, 3)

    slots(0, 36, first_layer)
    pl.run_scoped(
        lambda *bufs: slots(36, 54, lambda t: between(t, *bufs)),
        pltpu.VMEM((D, FF), BF16), pltpu.VMEM((D, FF), BF16), pltpu.VMEM((CF, FF), BF16), pltpu.VMEM((CF, FF), BF16),
    )
    slots(54, LAST, last_layer)
    last_waits()


def train(*operands):
    vm = pltpu.VMEM
    dma = pltpu.SemaphoreType.DMA
    any_, inside = pl.BlockSpec(memory_space=pl.ANY), pl.BlockSpec(memory_space=vm)
    shape = jax.ShapeDtypeStruct
    out_shape = [
        shape((CHUNKS, 2, 2, 4, ROWS, LANES), BF16), *[shape(t.shape, F32) for t in operands[3:9]],
        shape((72, OWN, T), BF16), shape((72, OWN, T), BF16),
        shape((T, FF), BF16), shape((T, FF), BF16),
    ]
    return pl.pallas_call(
        train_kernel,
        in_specs=[any_] * len(operands),
        out_specs=[any_, *[inside] * 4, *[any_] * (len(out_shape) - 5)],
        out_shape=out_shape,
        scratch_shapes=[
            vm((T, D), BF16), vm((T, D), BF16), vm((T, D), BF16), vm((D, T), BF16),
            vm((T, CF), BF16), vm((T, CF), BF16),
            vm((2, D, CF), BF16), vm((2, D, CF), BF16), vm((2, CF, D), BF16),
            vm((2, 8, OWN, T), BF16),
            vm((HELD, 2, 2, 4, ROWS, LANES), BF16), vm((HELD, 2, 4, ROWS, LANES), BF16),
            vm((RING, 5, ROWS, LANES), BF16),
            vm((OUT, 3, ROWS, LANES), BF16), vm((OUT, 3, ROWS, LANES), BF16),
            vm((RING, 4, ROWS, LANES), BF16), vm((ROWS, LANES), F32),
            vm((2, ROWS, LANES), F32), vm((2, ROWS, LANES), F32), vm((2, ROWS, LANES), BF16),
            vm((2, HALF, D), F32), vm((2, HALF, D), F32), vm((2, HALF, D), BF16),
            dma((3,)), dma((2, 3)), dma, dma((2,)), dma((2,)), dma((5,)),
            dma((2,)), dma((HELD,)), dma((SENDS,)), dma((RING,)), dma((SENDS,)), dma((RING,)),
            dma((SENDS,)), dma((RING,)), dma((SENDS,)), dma((RING,)), dma((SENDS,)), dma((RING,)),
            dma((SENDS,)), dma((RING,)), dma((SENDS,)), dma((RING,)), dma((SENDS,)), dma((2,)), dma((2, 3)),
        ],
        compiler_params=pltpu.CompilerParams(
            collective_id=0, has_side_effects=True, vmem_limit_bytes=VMEM_LIMIT
        ),
        name="train",
    )(*operands)


AHEAD = 12


def finish_kernel(
    wt, mg, mu, md, vg, vu, vd, owg, owu, owd, omg, omu, omd, ovg, ovu, ovd,
    wv, vuv, vdv, columns, rows, w_sem, in_sem, out_sem, col_sem, row_sem,
):
    moments = ((mg, omg), (mu, omu), (md, omd), (vg, ovg), (vuv, ovu), (vdv, ovd))
    pieces = [(i, layer) for layer in (1, 0) for i in range(6)]

    def take(layer):
        return [pltpu.make_async_copy(a.at[layer], b.at[layer], in_sem.at[i, layer]) for i, (a, b) in enumerate(((vu, vuv), (vd, vdv)))]

    def give(i, layer):
        return pltpu.make_async_copy(moments[i][0].at[layer], moments[i][1].at[layer], out_sem.at[i, layer])

    def chunk(p):
        return pltpu.make_async_copy(wt.at[p], wv.at[p % (AHEAD + 1)], w_sem.at[p % (AHEAD + 1)])

    def columns_out(out, layer, j, b):
        return pltpu.make_async_copy(columns.at[b], out.at[layer, :, pl.ds(pl.multiple_of(j * CF, CF), CF)], col_sem.at[b])

    def rows_out(layer, k, b):
        return pltpu.make_async_copy(rows.at[b], owd.at[layer, :, pl.ds(pl.multiple_of(k * OWN, OWN), OWN), :], row_sem.at[b])

    for p in range(AHEAD):
        chunk(p).start()

    def chunk_in(p):
        @pl.when(p + AHEAD < CHUNKS)
        def _():
            chunk(p + AHEAD).start()

        chunk(p).wait()

    for part in range(18):
        layer, base, n0 = 1 - part // 9, part // 9 * PER_LAYER, part % 9 * 3

        @pl.loop(0, 3)
        def _(i):
            n = n0 + i
            p = base + n
            chunk_in(p)
            e = p % (AHEAD + 1)
            if n0 < 18:
                b = n % 4

                @pl.when((n >= 4) | (base > 0))
                def _():
                    columns_out(owg, layer, 0, b).wait()

                for o in range(8):
                    for h in range(2):
                        columns[b, o * ROWS : (o + 1) * ROWS, h * LANES : (h + 1) * LANES] = wv[e, o % 2, h, o // 2]

                @pl.when(n % 2 == 0)
                def _():
                    columns_out(owg, layer, n // 2, b).start()

                @pl.when(n % 2 == 1)
                def _():
                    columns_out(owu, layer, n // 2, b).start()
            else:
                k = n - 18
                b = k % 4

                @pl.when((k >= 4) | (base > 0))
                def _():
                    rows_out(layer, 0, b).wait()

                for o in range(8):
                    for h in range(2):
                        for c in range(7):
                            rows[b, o, h * HALF : (h + 1) * HALF, c * LANES : (c + 1) * LANES] = wv[
                                e, o % 2, h, o // 2, c * HALF : (c + 1) * HALF, :
                            ]
                rows_out(layer, k, b).start()

        if part < 12:
            piece, side = pieces[part], part % 6
            if side == 0:
                for copy in take(piece[1]):
                    copy.start()
            if side == 4:
                for copy in take(piece[1]):
                    copy.wait()
            give(*piece).start()

    for b in range(4):
        columns_out(owg, 0, 0, b).wait()
        rows_out(0, 0, b).wait()
    for piece in pieces:
        give(*piece).wait()


def finish(wtmp, *moments):
    vm, dma = pltpu.VMEM, pltpu.SemaphoreType.DMA
    any_, inside = pl.BlockSpec(memory_space=pl.ANY), pl.BlockSpec(memory_space=vm)
    out = pl.pallas_call(
        finish_kernel,
        in_specs=[any_, *[inside] * 4, any_, any_],
        out_specs=[any_] * 9,
        out_shape=[
            jax.ShapeDtypeStruct((2, D, FF), BF16), jax.ShapeDtypeStruct((2, D, FF), BF16),
            jax.ShapeDtypeStruct((2, 8, 288, D), BF16),
            *[jax.ShapeDtypeStruct(t.shape, F32) for t in moments],
        ],
        scratch_shapes=[
            vm((AHEAD + 1, *wtmp.shape[1:]), BF16), vm(moments[4].shape, F32), vm(moments[5].shape, F32),
            vm((4, D, CF), BF16), vm((4, 8, OWN, D), BF16),
            dma((AHEAD + 1,)), dma((2, 2)), dma((6, 2)), dma((4,)), dma((4,)),
        ],
        compiler_params=pltpu.CompilerParams(vmem_limit_bytes=48000000),
        name="finish",
    )(wtmp, *moments)
    return (out[0], out[1], out[2].reshape(2, FF, D), *out[3:])


def solution(mesh):
    def step(x, dy, wg, wu, wd, *moments):
        out = train(wg, wu, wd, *moments, x[0], dy[0])
        return finish(*out[:7])

    seq, whole, rows = P(("rep", "dp")), P(), P(None, "dp")
    return jax.shard_map(
        step, mesh=mesh,
        in_specs=(seq, seq, *[whole] * 3, *[rows] * 6),
        out_specs=(*[P("rep")] * 3, *[P("rep", "dp")] * 6),
        check_vma=False,
    )
```
